64 devices in a mesh: rep: 8 (over x, y, core), dp: 8 (over z).
Axes of the slice: x: 2, y: 2, z: 8, core: 2. Of those that a mesh axis runs over, the one named last changes fastest.
The devices are a block of a 4x4x8 slice.
Arguments:
- x: bfloat16 [64, 4096, 512], P(('rep', 'dp')), parts along dimension 0
- dy: bfloat16 [64, 4096, 512], P(('rep', 'dp')), parts along dimension 0
- w_gate: bfloat16 [2, 512, 1408], replicated
- w_up: bfloat16 [2, 512, 1408], replicated
- w_down: bfloat16 [2, 1408, 512], replicated
- m_w_gate: float32 [2, 512, 1408], P(None, 'dp')
- m_w_up: float32 [2, 512, 1408], P(None, 'dp')
- m_w_down: float32 [2, 1408, 512], P(None, 'dp')
- v_w_gate: float32 [2, 512, 1408], P(None, 'dp')
- v_w_up: float32 [2, 512, 1408], P(None, 'dp')
- v_w_down: float32 [2, 1408, 512], P(None, 'dp')
Outputs:
- output 1: bfloat16 [16, 512, 1408], P('rep'), parts along dimension 0
- output 2: bfloat16 [16, 512, 1408], P('rep'), parts along dimension 0
- output 3: bfloat16 [16, 1408, 512], P('rep'), parts along dimension 0
- output 4: float32 [16, 512, 1408], P('rep', 'dp'), parts along dimension 0
- output 5: float32 [16, 512, 1408], P('rep', 'dp'), parts along dimension 0
- output 6: float32 [16, 1408, 512], P('rep', 'dp'), parts along dimension 0
- output 7: float32 [16, 512, 1408], P('rep', 'dp'), parts along dimension 0
- output 8: float32 [16, 512, 1408], P('rep', 'dp'), parts along dimension 0
- output 9: float32 [16, 1408, 512], P('rep', 'dp'), parts along dimension 0
There are 8 independent parts. The reference program is written for one: setup_inputs(seed, part) draws one part's arguments, and reference() takes and returns one part's arrays. A program takes and returns all parts, laid end to end along the dimension named above; an argument that names none is the same for every part.
All inputs are finite; a program needn't handle non-finite values.
Results may differ from the reference program's by a relative error of at most 0.022.
Values are sent between devices in bfloat16 or wider.
A program may use at most 768 MiB of HBM per device.

```python
import jax
import jax.numpy as jnp
from jax import lax

SEQUENCES = 8
TOKENS = 4096
D = 512
FF = 1408
LAYERS = 2
NAMES = ("w_gate", "w_up", "w_down")
SHAPES = {"w_gate": (LAYERS, D, FF), "w_up": (LAYERS, D, FF), "w_down": (LAYERS, FF, D)}


def bump(key, n, height):
    away = (jnp.arange(n, dtype=jnp.int32) - jax.random.randint(key, (), 0, n, jnp.int32)) % n
    return jnp.where(away < n // 8, height, 1.0)


def together(key, own, strength):
    shared = jax.random.normal(key, own.shape[1:], jnp.float32)
    return (own + strength * shared) * lax.rsqrt(1 + strength * strength)


def setup_inputs(seed: int = 0, part: int = 0) -> dict:
    kx, kdy, ka, kb, kz, kf, kh, kl, *keys = jax.random.split(jax.random.key(seed), 8 + 3 * len(NAMES))
    kx, kdy, ka, kb = (jax.random.fold_in(k, part) for k in (kx, kdy, ka, kb))
    kw, km, kv = (keys[i::3] for i in range(3))
    shape = (SEQUENCES, TOKENS, D)
    much_x, much_dy = jax.random.uniform(kz, (2,), jnp.float32, 0.0, 1.0)
    loud = 2.0 ** jax.random.uniform(jax.random.fold_in(kz, 1), (), jnp.float32, -1.0, 2.0)
    layers = 2.0 ** jax.random.uniform(kl, (LAYERS, 1, 1), jnp.float32, -1.0, 1.0)
    x = together(ka, jax.random.normal(kx, shape, jnp.float32), much_x) * bump(kf, D, 4.0)
    dy = together(kb, jax.random.normal(kdy, shape, jnp.float32), much_dy)
    drawn = {"x": x.astype(jnp.bfloat16), "dy": (loud * dy * (SEQUENCES * TOKENS) ** -0.5).astype(jnp.bfloat16)}
    for key, name in zip(kw, NAMES, strict=True):
        w = jax.random.normal(key, SHAPES[name], jnp.float32) * SHAPES[name][1] ** -0.5
        drawn[name] = (w * {"w_gate": 1.0, "w_up": bump(kh, FF, 4.0), "w_down": layers}[name]).astype(jnp.bfloat16)
    for key, name in zip(km, NAMES, strict=True):
        drawn[f"m_{name}"] = 0.1 * jax.random.normal(key, SHAPES[name], jnp.float32)
    for key, name in zip(kv, NAMES, strict=True):
        drawn[f"v_{name}"] = jax.random.uniform(key, SHAPES[name], jnp.float32, 0.005, 0.015)
    return drawn


def matmul(a, w):
    return jnp.dot(a, w, preferred_element_type=jnp.float32).astype(jnp.bfloat16)


def normed(h):
    wide = h.astype(jnp.float32)
    scale = lax.rsqrt(jnp.mean(wide**2, -1, keepdims=True) + 1e-6)
    return (wide * scale).astype(jnp.bfloat16)


def layer(h, w):
    a = normed(h)
    gate = jnp.dot(a, w["w_gate"], preferred_element_type=jnp.float32)
    up = jnp.dot(a, w["w_up"], preferred_element_type=jnp.float32)
    return h + matmul((jax.nn.silu(gate) * up).astype(jnp.bfloat16), w["w_down"])


def adamw(w, m, v, g):
    m = 0.9 * m + 0.1 * g
    v = 0.95 * v + 0.05 * g * g
    step = m * lax.rsqrt(v + 1e-8) + 0.1 * w
    return (w - 0.02 * step).astype(jnp.bfloat16), m, v


def clipped(gradients, sum_of_squares, count):
    factor = jnp.minimum(1.0, 0.5 * lax.rsqrt(sum_of_squares / count + 1e-30))
    return [g * factor for g in gradients]


def stack(weights, h):
    return lax.scan(lambda h, w: (layer(h, w), None), h, weights)[0]


def reference(x, dy, w_gate, w_up, w_down, m_w_gate, m_w_up, m_w_down, v_w_gate, v_w_up, v_w_down):
    weights = dict(zip(NAMES, (w_gate, w_up, w_down), strict=True))

    def take(so_far, sequence):
        h, by_y = sequence
        _, back = jax.vjp(lambda w: stack(w, h), weights)
        return jax.tree.map(lambda total, term: total + term.astype(jnp.float32), so_far, back(by_y)[0]), None

    none_yet = {name: jnp.zeros(w.shape, jnp.float32) for name, w in weights.items()}
    by_weights, _ = lax.scan(take, none_yet, (x, dy))
    gradients = [by_weights[name].astype(jnp.bfloat16).astype(jnp.float32) for name in NAMES]
    gradients = clipped(gradients, sum(jnp.sum(g * g) for g in gradients), sum(g.size for g in gradients))
    new = [
        adamw(w.astype(jnp.float32), m, v, g)
        for w, m, v, g in zip((w_gate, w_up, w_down), (m_w_gate, m_w_up, m_w_down), (v_w_gate, v_w_up, v_w_down), gradients, strict=True)
    ]
    return tuple(one[which] for which in range(3) for one in new)
```

```python
import jax
import jax.numpy as jnp
from jax import lax
from jax.sharding import PartitionSpec as P


def normed(h):
    wide = h.astype(jnp.float32)
    scale = lax.rsqrt(jnp.mean(wide**2, -1, keepdims=True) + 1e-6)
    return (wide * scale).astype(jnp.bfloat16)


def mid(gate, up):
    return (jax.nn.silu(gate) * up).astype(jnp.bfloat16)


def dot(a, b, dims):
    return lax.dot_general(a, b, (dims, ((), ())), preferred_element_type=jnp.float32)


def weight_grad(a, d):
    return dot(a, d, ((0,), (0,))).astype(jnp.bfloat16)


def adamw(w, m, v, g):
    m = 0.9 * m + 0.1 * g
    v = 0.95 * v + 0.05 * g * g
    step = m * lax.rsqrt(v + 1e-8) + 0.1 * w
    return (w - 0.02 * step).astype(jnp.bfloat16), m, v


def solution(mesh):
    n = mesh.shape["dp"]

    def scatter(g):
        return lax.psum_scatter(g, "dp", scatter_dimension=0, tiled=True)

    def step(x, dy, wg, wu, wd, mg, mu, md, vg, vu, vd):
        x, dy = x[0], dy[0]
        layers = wg.shape[0]
        saved = []
        h = x
        for i in range(layers):
            a, norm_back = jax.vjp(normed, h)
            gate, up = dot(a, wg[i], ((1,), (0,))), dot(a, wu[i], ((1,), (0,)))
            s, mid_back = jax.vjp(mid, gate, up)
            saved.append((a, norm_back, s, mid_back))
            if i < layers - 1:
                h = h + dot(s, wd[i], ((1,), (0,))).astype(jnp.bfloat16)
        shards = [None] * layers
        dh = dy
        for i in reversed(range(layers)):
            a, norm_back, s, mid_back = saved[i]
            down = scatter(weight_grad(s, dh))
            ds = dot(dh, wd[i], ((1,), (1,))).astype(jnp.bfloat16)
            dgate, dup = (t.astype(jnp.bfloat16) for t in mid_back(ds))
            gate_shard = scatter(weight_grad(a, dgate))
            up_shard = scatter(weight_grad(a, dup))
            shards[i] = (gate_shard, up_shard, down)
            if i > 0:
                da = dot(dgate, wg[i], ((1,), (1,))).astype(jnp.bfloat16) + dot(dup, wu[i], ((1,), (1,))).astype(jnp.bfloat16)
                dh = dh + norm_back(da)[0]
        grads = [[s.astype(jnp.float32) for s in layer] for layer in shards]
        total = lax.psum(sum(jnp.sum(g * g) for layer in grads for g in layer), "dp")
        count = sum(w.size for w in (wg, wu, wd))
        factor = jnp.minimum(1.0, 0.5 * lax.rsqrt(total / count + 1e-30))
        me = lax.axis_index("dp")
        new_w, new_m, new_v = [], [], []
        for k, (w, m, v) in enumerate(((wg, mg, vg), (wu, mu, vu), (wd, md, vd))):
            rows = w.shape[1] // n
            out = []
            for i in range(layers):
                mine = lax.dynamic_slice_in_dim(w[i], me * rows, rows, 0).astype(jnp.float32)
                nw, nm, nv = adamw(mine, m[i], v[i], grads[i][k] * factor)
                out.append((lax.all_gather(nw, "dp", axis=0, tiled=True), nm, nv))
            for lst, vals in zip((new_w, new_m, new_v), zip(*out)):
                lst.append(jnp.stack(vals))
        return (*new_w, *new_m, *new_v)

    seq, whole, rows = P(("rep", "dp"), None, None), P(None, None, None), P(None, "dp", None)
    return jax.shard_map(
        step,
        mesh=mesh,
        in_specs=(seq, seq) + (whole,) * 3 + (rows,) * 6,
        out_specs=(P("rep", None, None),) * 3 + (P("rep", "dp", None),) * 6,
        check_vma=False,
    )
```

```python
import functools

import jax
import jax.numpy as jnp
from jax import lax
from jax.experimental import pallas as pl
from jax.experimental.pallas import tpu as pltpu
from jax.sharding import PartitionSpec as P

BF, F32 = jnp.bfloat16, jnp.float32
MESH = pl.DeviceIdType.MESH
ANY = pl.BlockSpec(memory_space=pl.ANY)
ROWS = (((1,), (0,)), ((), ()))
BY_T = (((1,), (1,)), ((), ()))
T_BY = (((0,), (0,)), ((), ()))


def dot(a, b, dims):
    return lax.dot_general(a, b, dims, preferred_element_type=F32)


def rms_scale(wide):
    return lax.rsqrt(jnp.mean(wide * wide, -1, keepdims=True) + 1e-6)


def sigmoid(t):
    return 1.0 / (1.0 + jnp.exp(-t))


class Ring:
    def __init__(self, n, own, recv, send_sem, recv_sem):
        self.n, self.own, self.recv, self.send_sem, self.recv_sem = n, own, recv, send_sem, recv_sem
        self.rows, self.half = recv.shape[2], recv.shape[3]
        far, near = n // 2, n - 1 - n // 2
        self.streams = ((0, 1, far), (1, -1, far), (1, 1, near), (0, -1, near))
        self.me = lax.axis_index("dp")

    def mine(self, owner, half):
        owner = lax.rem(owner + self.n, self.n)
        rows = pl.ds(pl.multiple_of(owner * self.rows, self.rows), self.rows)
        return self.own.at[rows, pl.ds(half * self.half, self.half)]

    def copy(self, s, hop):
        half, way, hops = self.streams[s]
        src = self.mine(self.me + way * hops, half) if hop == 1 else self.recv.at[s, hop - 2]
        to = lax.rem(self.me + way + self.n, self.n)
        return pltpu.make_async_remote_copy(
            src_ref=src,
            dst_ref=self.recv.at[s, hop - 1],
            send_sem=self.send_sem.at[s, hop - 1],
            recv_sem=self.recv_sem.at[s, hop - 1],
            device_id={"dp": to},
            device_id_type=MESH,
        )

    def start(self):
        for s in range(4):
            self.copy(s, 1).start()

    def add(self, s, hop):
        half, way, hops = self.streams[s]
        self.copy(s, hop).wait_recv()
        if hop < hops:
            buf = self.recv.at[s, hop - 1]
            term = self.mine(self.me + way * (hops - hop), half)
            buf[...] = (buf[...].astype(F32) + term[...].astype(F32)).astype(BF)

    def send(self, s, hop):
        if hop < self.streams[s][2]:
            self.copy(s, hop + 1).start()

    def events(self):
        out = []
        for hop in range(1, self.streams[0][2] + 1):
            for pair in ((0, 1), (2, 3)):
                if hop <= self.streams[pair[0]][2]:
                    out.append(tuple((s, hop) for s in pair))
        return out

    def handle(self, pair):
        for s, hop in pair:
            self.add(s, hop)
        for s, hop in pair:
            self.send(s, hop)

    def finish(self, out):
        for half in (0, 1):
            total = self.mine(self.me, half)[...].astype(F32)
            for s, (its, _, hops) in enumerate(self.streams):
                if its == half:
                    total = total + self.recv[s, hops - 1].astype(F32)
            out[:, pl.ds(half * self.half, self.half)] = total.astype(BF)
        for s, (_, _, hops) in enumerate(self.streams):
            for hop in range(1, hops + 1):
                self.copy(s, hop).wait_send()


def ring_scratch(n, rows, cols):
    return [
        pltpu.VMEM((n * rows, cols), BF),
        pltpu.VMEM((4, n // 2, rows, cols // 2), BF),
        pltpu.SemaphoreType.DMA((4, n // 2)),
        pltpu.SemaphoreType.DMA((4, n // 2)),
        pltpu.SemaphoreType.DMA(()),
    ]


def greet(n, others):
    me = lax.axis_index("dp")
    barrier = pltpu.get_barrier_semaphore()
    for d in others:
        pl.semaphore_signal(barrier, inc=1, device_id={"dp": lax.rem(me + d + n, n)}, device_id_type=MESH)
    pl.semaphore_wait(barrier, len(others))


def with_ring(n, steps, due, refs, own_hbm, out):
    own, recv, send_sem, recv_sem, load_sem = refs
    i = pl.program_id(0)
    ring = Ring(n, own, recv, send_sem, recv_sem)
    load = pltpu.make_async_copy(own_hbm, own, load_sem)

    @pl.when(i == 0)
    def _():
        load.start()
        greet(n, (1, -1))
        load.wait()
        ring.start()

    events = ring.events()
    for step in range(1, steps):
        now = [e for e, d in zip(events, due, strict=True) if d == step]
        if now:

            @pl.when(i == step)
            def _(now=now):
                for e in now:
                    ring.handle(e)

    def close():
        @pl.when(i == steps - 1)
        def _():
            for e, d in zip(events, due, strict=True):
                if d >= steps:
                    ring.handle(e)
            ring.finish(out)

    return close


def load_all(copies):
    @pl.when(pl.program_id(0) == 0)
    def _():
        for c in copies:
            c.start()
        for c in copies:
            c.wait()


def top_kernel(x_ref, dy_ref, wg, wu, wd, gu0_ref, h1_ref, dgu1_ref, dwd_ref, wgu, wdn, acc, sem):
    i = pl.program_id(0)
    ff = wd.shape[1]
    load_all(
        [pltpu.make_async_copy(wg.at[k], wgu.at[k, :, pl.ds(0, ff)], sem.at[k, 0]) for k in (0, 1)]
        + [pltpu.make_async_copy(wu.at[k], wgu.at[k, :, pl.ds(ff, ff)], sem.at[k, 1]) for k in (0, 1)]
        + [pltpu.make_async_copy(wd.at[k], wdn.at[k], sem.at[k, 2]) for k in (0, 1)]
    )
    x = x_ref[...].astype(F32)
    gu = dot((x * rms_scale(x)).astype(BF), wgu[0], ROWS)
    gu0_ref[...] = gu
    gate, up = gu[:, :ff], gu[:, ff:]
    s = (gate * sigmoid(gate) * up).astype(BF)
    h = (x + dot(s, wdn[0], ROWS).astype(BF).astype(F32)).astype(BF)
    h1_ref[...] = h
    h = h.astype(F32)
    gu = dot((h * rms_scale(h)).astype(BF), wgu[1], ROWS)
    gate, up = gu[:, :ff], gu[:, ff:]
    sig = sigmoid(gate)
    silu = gate * sig
    dy = dy_ref[...]
    part = dot((silu * up).astype(BF), dy, T_BY)

    @pl.when(i == 0)
    def _():
        acc[...] = part

    @pl.when(i > 0)
    def _():
        acc[...] += part

    ds = dot(dy, wdn[1], BY_T).astype(BF).astype(F32)
    dgu1_ref[:, :ff] = (ds * up * (sig + silu * (1.0 - sig))).astype(BF)
    dgu1_ref[:, ff:] = (ds * silu).astype(BF)

    @pl.when(i == pl.num_programs(0) - 1)
    def _():
        dwd_ref[...] = acc[...].astype(BF)


def gu_kernel(n, due, h_ref, dgu_ref, own_hbm, dw_ref, sum_ref, acc, *ring):
    i = pl.program_id(0)
    close = with_ring(n, len(due[1]), due[0], ring, own_hbm, sum_ref)
    h = h_ref[...].astype(F32)
    part = dot((h * rms_scale(h)).astype(BF), dgu_ref[...], T_BY)

    @pl.when(i == 0)
    def _():
        acc[...] = part

    @pl.when(i > 0)
    def _():
        acc[...] += part

    @pl.when(i == pl.num_programs(0) - 1)
    def _():
        dw_ref[...] = acc[...].astype(BF)

    close()


def mid_kernel(n, due, h1_ref, dy_ref, dgu1_ref, gu0_ref, wg, wu, wd, own_hbm, dgu0_ref, dwd_ref, sum_ref, wgu, wdn, acc, sem, *ring):
    i = pl.program_id(0)
    ff = wd.shape[1]
    close = with_ring(n, len(due[1]), due[0], ring, own_hbm, sum_ref)
    load_all(
        [
            pltpu.make_async_copy(wg.at[1], wgu.at[:, pl.ds(0, ff)], sem.at[0]),
            pltpu.make_async_copy(wu.at[1], wgu.at[:, pl.ds(ff, ff)], sem.at[1]),
            pltpu.make_async_copy(wd.at[0], wdn, sem.at[2]),
        ]
    )
    da = dot(dgu1_ref[...], wgu[...], BY_T).astype(BF).astype(F32)
    h = h1_ref[...].astype(F32)
    scale = rms_scale(h)
    back = scale * (da - h * (scale * scale * jnp.mean(da * h, -1, keepdims=True)))
    dh = (dy_ref[...].astype(F32) + back.astype(BF).astype(F32)).astype(BF)
    ds = dot(dh, wdn[...], BY_T).astype(BF).astype(F32)
    gate, up = gu0_ref[:, :ff], gu0_ref[:, ff:]
    sig = sigmoid(gate)
    silu = gate * sig
    dgu0_ref[:, :ff] = (ds * up * (sig + silu * (1.0 - sig))).astype(BF)
    dgu0_ref[:, ff:] = (ds * silu).astype(BF)
    part = dot((silu * up).astype(BF), dh, T_BY)

    @pl.when(i == 0)
    def _():
        acc[...] = part

    @pl.when(i > 0)
    def _():
        acc[...] += part

    @pl.when(i == pl.num_programs(0) - 1)
    def _():
        dwd_ref[...] = acc[...].astype(BF)

    close()


def end_kernel(
    n, count, gu1, d1, d0, own_hbm, wg, wu, wd, mg, mu, md, vg, vu, vd,
    owg, owu, owd, omg, omu, omd, ovg, ovu, ovd,
    gbuf, dbuf, all_g, all_u, all_d, mb_g, mb_d, vb_g, vb_d, wb_g, wb_d, sq_send, sq_all,
    in_sem, out_sem, sq_s, sq_r, ag_s, ag_r, *ring_refs,
):
    me = lax.axis_index("dp")
    ff, d = md.shape[1] * n, md.shape[2]
    rg, rd = mg.shape[1], md.shape[1]
    own, recv, send_sem, recv_sem, load_sem = ring_refs
    ring = Ring(n, own, recv, send_sem, recv_sem)
    my_g = pl.ds(pl.multiple_of(me * rg, rg), rg)
    my_d = pl.ds(pl.multiple_of(me * rd, rd), rd)
    load = pltpu.make_async_copy(own_hbm, own, load_sem)
    load.start()
    loads = [
        pltpu.make_async_copy(gu1, gbuf.at[1], in_sem.at[0]),
        pltpu.make_async_copy(d1, dbuf.at[1], in_sem.at[1]),
        pltpu.make_async_copy(d0, dbuf.at[0], in_sem.at[2]),
        pltpu.make_async_copy(mg, mb_g.at[0], in_sem.at[3]),
        pltpu.make_async_copy(mu, mb_g.at[1], in_sem.at[4]),
        pltpu.make_async_copy(md, mb_d, in_sem.at[5]),
        pltpu.make_async_copy(vg, vb_g.at[0], in_sem.at[6]),
        pltpu.make_async_copy(vu, vb_g.at[1], in_sem.at[7]),
        pltpu.make_async_copy(vd, vb_d, in_sem.at[8]),
        pltpu.make_async_copy(wg.at[:, my_g], wb_g.at[0], in_sem.at[9]),
        pltpu.make_async_copy(wu.at[:, my_g], wb_g.at[1], in_sem.at[10]),
        pltpu.make_async_copy(wd.at[:, my_d], wb_d, in_sem.at[11]),
    ]
    for c in loads:
        c.start()
    greet(n, tuple(range(1, n)))
    load.wait()
    ring.start()
    for c in loads:
        c.wait()
    for e in ring.events():
        ring.handle(e)
    ring.finish(gbuf.at[0])

    def squares(t):
        t = t.astype(F32)
        t = t * t
        t = jnp.sum(t.reshape(t.shape[0] // 8, 8, t.shape[1]), 0)
        return sum(t[:, k : k + 128] for k in range(0, t.shape[1], 128))

    sq = squares(gbuf[0]) + squares(gbuf[1]) + squares(dbuf[0]) + squares(dbuf[1])
    sq_send[...] = sq
    to_all = [
        pltpu.make_async_remote_copy(
            src_ref=sq_send,
            dst_ref=sq_all.at[k - 1],
            send_sem=sq_s.at[k - 1],
            recv_sem=sq_r.at[k - 1],
            device_id={"dp": lax.rem(me + k, n)},
            device_id_type=MESH,
        )
        for k in range(1, n)
    ]
    for c in to_all:
        c.start()
    for c in to_all:
        c.wait_recv()
    total = jnp.sum(sq + jnp.sum(sq_all[...], 0), keepdims=True)
    factor = jnp.minimum(1.0, 0.5 * lax.rsqrt(total / count + 1e-30))

    far, near = n // 2, n - 1 - n // 2
    streams = ((0, 1, far), (1, -1, far), (1, 1, near), (0, -1, near))

    def gathered(layer, down, half, owner):
        owner = lax.rem(owner + n, n)
        if down:
            return all_d.at[layer, pl.ds(pl.multiple_of(owner * rd, rd), rd), pl.ds(half * (d // 2), d // 2)]
        return (all_g, all_u)[half].at[layer, pl.ds(pl.multiple_of(owner * rg, rg), rg)]

    def copy(layer, down, s, hop):
        half, way, _ = streams[s]
        part = gathered(layer, down, half, me - way * (hop - 1))
        unit = layer * 2 + down
        return pltpu.make_async_remote_copy(
            src_ref=part,
            dst_ref=part,
            send_sem=ag_s.at[unit, s, hop - 1],
            recv_sem=ag_r.at[unit, s, hop - 1],
            device_id={"dp": lax.rem(me + way + n, n)},
            device_id_type=MESH,
        )

    def arrival(layer, down, s, hop):
        half, way, _ = streams[s]
        part = gathered(layer, down, half, me - way * hop)
        unit = layer * 2 + down
        return pltpu.make_async_remote_copy(
            src_ref=part,
            dst_ref=part,
            send_sem=ag_s.at[unit, s, hop - 1],
            recv_sem=ag_r.at[unit, s, hop - 1],
            device_id={"dp": lax.rem(me + way + n, n)},
            device_id_type=MESH,
        )

    def adamw(w_ref, m_ref, v_ref, g, out):
        g = g.astype(F32) * factor
        m = 0.9 * m_ref[...] + 0.1 * g
        v = 0.95 * v_ref[...] + 0.05 * g * g
        w = w_ref[...].astype(F32)
        out[...] = (w - 0.02 * (m * lax.rsqrt(v + 1e-8) + 0.1 * w)).astype(BF)
        m_ref[...] = m
        v_ref[...] = v

    units = [(layer, down) for layer in (0, 1) for down in (0, 1)]
    for layer, down in units:
        if down:
            adamw(wb_d.at[layer], mb_d.at[layer], vb_d.at[layer], dbuf[layer], all_d.at[layer, my_d])
        else:
            for k, to in ((0, all_g), (1, all_u)):
                adamw(wb_g.at[k, layer], mb_g.at[k, layer], vb_g.at[k, layer], gbuf[layer, :, k * ff : (k + 1) * ff], to.at[layer, my_g])
        for s in range(4):
            copy(layer, down, s, 1).start()
    stores = [
        pltpu.make_async_copy(a, b, out_sem.at[k])
        for k, (a, b) in enumerate(
            ((mb_g.at[0], omg), (mb_g.at[1], omu), (mb_d, omd), (vb_g.at[0], ovg), (vb_g.at[1], ovu), (vb_d, ovd))
        )
    ]
    for c in stores:
        c.start()
    for hop in range(1, far + 1):
        for layer, down in units:
            for s in range(4):
                if hop <= streams[s][2]:
                    arrival(layer, down, s, hop).wait_recv()
                    if hop < streams[s][2]:
                        copy(layer, down, s, hop + 1).start()
    last = [pltpu.make_async_copy(a, b, out_sem.at[6 + k]) for k, (a, b) in enumerate(((all_g, owg), (all_u, owu), (all_d, owd)))]
    for c in last:
        c.start()
    for c in to_all:
        c.wait_send()
    for layer, down in units:
        for s in range(4):
            for hop in range(1, streams[s][2] + 1):
                copy(layer, down, s, hop).wait_send()
    for c in stores + last:
        c.wait()


def params(cid=None):
    if cid is None:
        return pltpu.CompilerParams(vmem_limit_bytes=62 << 20, dimension_semantics=("arbitrary",))
    return pltpu.CompilerParams(vmem_limit_bytes=62 << 20, collective_id=cid, has_side_effects=True)


def solution(mesh):
    n = mesh.shape["dp"]

    def step(x, dy, wg, wu, wd, mg, mu, md, vg, vu, vd):
        x, dy = x[0], dy[0]
        tokens, d = x.shape
        ff = wd.shape[1]
        rg, rd = d // n, ff // n
        tile = 256
        steps = tokens // tile
        rows = lambda c: pl.BlockSpec((tile, c), lambda i: (i, 0))
        whole = lambda *s: pl.BlockSpec(s, lambda i: (0,) * len(s))
        array = jax.ShapeDtypeStruct
        sem = pltpu.SemaphoreType.DMA
        mm = 2 * tokens * d * ff

        gu0, h1, dgu1, dwd1 = pl.pallas_call(
            top_kernel,
            grid=(steps,),
            in_specs=[rows(d), rows(d), ANY, ANY, ANY],
            out_specs=[rows(2 * ff), rows(d), rows(2 * ff), whole(ff, d)],
            out_shape=[array((tokens, 2 * ff), F32), array((tokens, d), BF), array((tokens, 2 * ff), BF), array((ff, d), BF)],
            scratch_shapes=[pltpu.VMEM((2, d, 2 * ff), BF), pltpu.VMEM((2, ff, d), BF), pltpu.VMEM((ff, d), F32), sem((2, 3))],
            compiler_params=params(),
            cost_estimate=pl.CostEstimate(flops=7 * mm, bytes_accessed=90 << 20, transcendentals=0),
            name="top",
        )(x, dy, wg, wu, wd)

        def due(msg_us, step_us):
            at = [2.5 + (p + 1) * msg_us for p in range(n - 1)]
            return [int(t / step_us) + 1 for t in at], [0] * steps

        def gu_grad(h, dgu, own, cid, name):
            return pl.pallas_call(
                functools.partial(gu_kernel, n, due(1.95, 1.0)),
                grid=(steps,),
                in_specs=[rows(d), rows(2 * ff), ANY],
                out_specs=[whole(d, 2 * ff), whole(rd, d)],
                out_shape=[array((d, 2 * ff), BF), array((rd, d), BF)],
                scratch_shapes=[pltpu.VMEM((d, 2 * ff), F32)] + ring_scratch(n, rd, d),
                compiler_params=params(cid),
                cost_estimate=pl.CostEstimate(flops=2 * mm, bytes_accessed=30 << 20, transcendentals=0),
                name=name,
            )(h, dgu, own)

        dwgu1, sum_d1 = gu_grad(h1, dgu1, dwd1, 0, "gu1")
        dgu0, dwd0, sum_gu1 = pl.pallas_call(
            functools.partial(mid_kernel, n, due(3.87, 2.0)),
            grid=(steps,),
            in_specs=[rows(d), rows(d), rows(2 * ff), rows(2 * ff), ANY, ANY, ANY, ANY],
            out_specs=[rows(2 * ff), whole(ff, d), whole(rg, 2 * ff)],
            out_shape=[array((tokens, 2 * ff), BF), array((ff, d), BF), array((rg, 2 * ff), BF)],
            scratch_shapes=[pltpu.VMEM((d, 2 * ff), BF), pltpu.VMEM((ff, d), BF), pltpu.VMEM((ff, d), F32), sem((3,))]
            + ring_scratch(n, rg, 2 * ff),
            compiler_params=params(1),
            cost_estimate=pl.CostEstimate(flops=4 * mm, bytes_accessed=100 << 20, transcendentals=0),
            name="mid",
        )(h1, dy, dgu1, gu0, wg, wu, wd, dwgu1)
        dwgu0, sum_d0 = gu_grad(x, dgu0, dwd0, 2, "gu0")

        vm = pltpu.VMEM
        outs = pl.pallas_call(
            functools.partial(end_kernel, n, float(wg.size + wu.size + wd.size)),
            in_specs=[ANY] * 13,
            out_specs=[ANY] * 9,
            out_shape=[array(t.shape, BF) for t in (wg, wu, wd)] + [array(t.shape, F32) for t in (mg, mu, md, vg, vu, vd)],
            scratch_shapes=[
                vm((2, rg, 2 * ff), BF), vm((2, rd, d), BF),
                vm(wg.shape, BF), vm(wu.shape, BF), vm(wd.shape, BF),
                vm((2, *mg.shape), F32), vm(md.shape, F32), vm((2, *vg.shape), F32), vm(vd.shape, F32),
                vm((2, *mg.shape), BF), vm(md.shape, BF),
                vm((8, 128), F32), vm((n - 1, 8, 128), F32),
                sem((12,)), sem((9,)), sem((n - 1,)), sem((n - 1,)), sem((4, 4, n // 2)), sem((4, 4, n // 2)),
            ] + ring_scratch(n, rg, 2 * ff),
            compiler_params=params(3),
            name="end",
        )(sum_gu1, sum_d1, sum_d0, dwgu0, wg, wu, wd, mg, mu, md, vg, vu, vd)
        return tuple(outs)

    seq, whole, rows = P(("rep", "dp"), None, None), P(None, None, None), P(None, "dp", None)
    return jax.shard_map(
        step,
        mesh=mesh,
        in_specs=(seq, seq) + (whole,) * 3 + (rows,) * 6,
        out_specs=(P("rep", None, None),) * 3 + (P("rep", "dp", None),) * 6,
        check_vma=False,
    )
```

```python
import functools

import jax
import jax.numpy as jnp
from jax import lax
from jax.experimental import pallas as pl
from jax.experimental.pallas import tpu as pltpu
from jax.sharding import PartitionSpec as P

BF, F32 = jnp.bfloat16, jnp.float32
MESH = pl.DeviceIdType.MESH
ANY = pl.BlockSpec(memory_space=pl.ANY)
ROWS = (((1,), (0,)), ((), ()))
BY_T = (((1,), (1,)), ((), ()))
T_BY = (((0,), (0,)), ((), ()))


def dot(a, b, dims):
    return lax.dot_general(a, b, dims, preferred_element_type=F32)


def rms_scale(wide):
    return lax.rsqrt(jnp.mean(wide * wide, -1, keepdims=True) + 1e-6)


def sigmoid(t):
    return 1.0 / (1.0 + jnp.exp(-t))


class Ring:
    def __init__(self, n, own, recv, send_sem, recv_sem):
        self.n, self.own, self.recv, self.send_sem, self.recv_sem = n, own, recv, send_sem, recv_sem
        self.rows, self.half = recv.shape[2], recv.shape[3]
        far, near = n // 2, n - 1 - n // 2
        self.streams = ((0, 1, far), (1, -1, far), (1, 1, near), (0, -1, near))
        self.me = lax.axis_index("dp")

    def mine(self, owner, half):
        owner = lax.rem(owner + self.n, self.n)
        rows = pl.ds(pl.multiple_of(owner * self.rows, self.rows), self.rows)
        return self.own.at[rows, pl.ds(half * self.half, self.half)]

    def copy(self, s, hop):
        half, way, hops = self.streams[s]
        src = self.mine(self.me + way * hops, half) if hop == 1 else self.recv.at[s, hop - 2]
        to = lax.rem(self.me + way + self.n, self.n)
        return pltpu.make_async_remote_copy(
            src_ref=src,
            dst_ref=self.recv.at[s, hop - 1],
            send_sem=self.send_sem.at[s, hop - 1],
            recv_sem=self.recv_sem.at[s, hop - 1],
            device_id={"dp": to},
            device_id_type=MESH,
        )

    def start(self):
        for s in range(4):
            self.copy(s, 1).start()

    def add(self, s, hop):
        half, way, hops = self.streams[s]
        self.copy(s, hop).wait_recv()
        if hop < hops:
            buf = self.recv.at[s, hop - 1]
            term = self.mine(self.me + way * (hops - hop), half)
            buf[...] = (buf[...].astype(F32) + term[...].astype(F32)).astype(BF)

    def send(self, s, hop):
        if hop < self.streams[s][2]:
            self.copy(s, hop + 1).start()

    def handle(self, pair):
        for s, hop in pair:
            self.add(s, hop)
        for s, hop in pair:
            self.send(s, hop)

    def finish(self, out):
        for half in (0, 1):
            total = self.mine(self.me, half)[...].astype(F32)
            for s, (its, _, hops) in enumerate(self.streams):
                if its == half:
                    total = total + self.recv[s, hops - 1].astype(F32)
            out[:, pl.ds(half * self.half, self.half)] = total.astype(BF)
        for s, (_, _, hops) in enumerate(self.streams):
            for hop in range(1, hops + 1):
                self.copy(s, hop).wait_send()


def greet(n, others):
    me = lax.axis_index("dp")
    barrier = pltpu.get_barrier_semaphore()
    for d in others:
        pl.semaphore_signal(barrier, inc=1, device_id={"dp": lax.rem(me + d + n, n)}, device_id_type=MESH)
    pl.semaphore_wait(barrier, len(others))


def plan(hops, rings, steps, step_us):
    latency, free, waiting, out = 2.5, 0.0, [], []
    far, near = hops

    def send(ring, group, hop, now):
        nonlocal free
        free = max(free, now) + rings[ring][1]
        waiting.append((free + latency, ring, group, hop))

    step, now = 0, 0.0
    while step < steps or waiting:
        if step < steps:
            now = step * step_us
        else:
            now = max(steps * step_us, min(w[0] for w in waiting))
        for w in sorted(w for w in waiting if w[0] <= now):
            waiting.remove(w)
            _, ring, group, hop = w
            out.append((min(step, steps), ring, tuple((s, hop) for s in ((0, 1), (2, 3))[group])))
            if hop < (far, near)[group]:
                send(ring, group, hop + 1, now)
        for ring, (start, _) in enumerate(rings):
            if start == step:
                send(ring, 0, 1, now)
                send(ring, 1, 1, now)
        step += 1
    return out


def run_plan(todo, rings, steps):
    i = pl.program_id(0)
    for step in range(1, steps):
        now = [(r, pair) for at, r, pair in todo if at == step]
        if now:

            @pl.when(i == step)
            def _(now=now):
                for r, pair in now:
                    rings[r].handle(pair)


def rest_of_plan(todo, rings, steps):
    for at, r, pair in todo:
        if at >= steps:
            rings[r].handle(pair)


def with_ring(n, steps, todo, refs, own_hbm, out):
    own, load_sem, recv, send_sem, recv_sem = refs
    i = pl.program_id(0)
    ring = Ring(n, own, recv, send_sem, recv_sem)
    load = pltpu.make_async_copy(own_hbm, own, load_sem)

    @pl.when(i == 0)
    def _():
        load.start()
        greet(n, (1, -1))
        load.wait()
        ring.start()

    run_plan(todo, [ring], steps)

    def close():
        @pl.when(i == steps - 1)
        def _():
            rest_of_plan(todo, [ring], steps)
            ring.finish(out)

    return close


def load_all(copies):
    @pl.when(pl.program_id(0) == 0)
    def _():
        for c in copies:
            c.start()
        for c in copies:
            c.wait()


LANES = 128


def gate_up_copies(wg, wu, wgu, sem, blocks):
    out = []
    for k in range(blocks):
        for j, w in enumerate((wg, wu)):
            to = wgu.at[:, pl.ds(LANES * (2 * k + j), LANES)]
            out.append(pltpu.make_async_copy(w.at[:, pl.ds(LANES * k, LANES)], to, sem.at[2 * k + j]))
    return out


def chunks(blocks):
    return [(k, min(2, blocks - k)) for k in range(0, blocks, 2)]


def halves(ref):
    rows = ref.shape[0] // 2
    return [pl.ds(0, rows), pl.ds(rows, rows)]


def gated(gate, up, ds):
    sig = sigmoid(gate)
    silu = gate * sig
    ds = ds.astype(BF).astype(F32)
    return (silu * up).astype(BF), (ds * up * (sig + silu * (1.0 - sig))).astype(BF), (ds * silu).astype(BF)


def top_kernel(x_ref, dy_ref, wg, wu, wd, gu0_ref, h1_ref, a0_ref, a1_ref, dgu1_ref, dwd_ref, wgu, wdn, s_ref, acc, sem, dsem):
    i = pl.program_id(0)
    blocks = wd.shape[1] // LANES
    load_all(
        [c for k in (0, 1) for c in gate_up_copies(wg.at[k], wu.at[k], wgu.at[k], sem.at[k], blocks)]
        + [pltpu.make_async_copy(wd.at[k], wdn.at[k], dsem.at[k]) for k in (0, 1)]
    )

    @pl.when(i == 0)
    def _():
        acc[...] = jnp.zeros_like(acc)

    rows = halves(x_ref)
    for r in rows:
        x = x_ref[r, :].astype(F32)
        a0_ref[r, :] = (x * rms_scale(x)).astype(BF)
    for k, c in chunks(blocks):
        at = pl.ds(2 * LANES * k, 2 * LANES * c)
        for r in rows:
            gu = dot(a0_ref[r, :], wgu[0, :, at], ROWS)
            gu0_ref[r, at] = gu
            for b in range(c):
                gate, up = (gu[:, (2 * b + j) * LANES : (2 * b + j + 1) * LANES] for j in (0, 1))
                s_ref[r, pl.ds((k + b) * LANES, LANES)] = (gate * sigmoid(gate) * up).astype(BF)
    for r in rows:
        h = x_ref[r, :].astype(F32) + dot(s_ref[r, :], wdn[0], ROWS).astype(BF).astype(F32)
        h = h.astype(BF)
        h1_ref[r, :] = h
        h = h.astype(F32)
        a1_ref[r, :] = (h * rms_scale(h)).astype(BF)
    for k, c in chunks(blocks):
        at = pl.ds(2 * LANES * k, 2 * LANES * c)
        for r in rows:
            gu = dot(a1_ref[r, :], wgu[1, :, at], ROWS)
            ds = dot(dy_ref[r, :], wdn[1, pl.ds(LANES * k, LANES * c), :], BY_T)
            for b in range(c):
                gate, up = (gu[:, (2 * b + j) * LANES : (2 * b + j + 1) * LANES] for j in (0, 1))
                s, dgate, dup = gated(gate, up, ds[:, b * LANES : (b + 1) * LANES])
                s_ref[r, pl.ds((k + b) * LANES, LANES)] = s
                dgu1_ref[r, pl.ds(2 * (k + b) * LANES, LANES)] = dgate
                dgu1_ref[r, pl.ds((2 * (k + b) + 1) * LANES, LANES)] = dup
    acc[...] += dot(s_ref[...], dy_ref[...], T_BY)

    @pl.when(i == pl.num_programs(0) - 1)
    def _():
        dwd_ref[...] = acc[...].astype(BF)


def gu_kernel(n, steps, todo, a_ref, dgu_ref, own_hbm, dw_ref, sum_ref, *ring):
    close = with_ring(n, steps, todo, ring, own_hbm, sum_ref)
    dw_ref[...] = dot(a_ref[...], dgu_ref[...], T_BY).astype(BF)
    close()


def mid_kernel(
    n, steps, todo, h1_ref, dy_ref, dgu1_ref, gu0_ref, wg, wu, wd, own_hbm, dgu0_ref, dwd_ref, sum_ref,
    wgu, wdn, s_ref, dh_ref, acc, sem, dsem, *ring,
):
    i = pl.program_id(0)
    blocks = wd.shape[1] // LANES
    close = with_ring(n, steps, todo, ring, own_hbm, sum_ref)
    load_all(gate_up_copies(wg.at[1], wu.at[1], wgu, sem, blocks) + [pltpu.make_async_copy(wd.at[0], wdn, dsem)])

    @pl.when(i == 0)
    def _():
        acc[...] = jnp.zeros_like(acc)

    rows = halves(h1_ref)
    for r in rows:
        da = dot(dgu1_ref[r, :], wgu[...], BY_T).astype(BF).astype(F32)
        h = h1_ref[r, :].astype(F32)
        scale = rms_scale(h)
        back = scale * (da - h * (scale * scale * jnp.mean(da * h, -1, keepdims=True)))
        dh_ref[r, :] = (dy_ref[r, :].astype(F32) + back.astype(BF).astype(F32)).astype(BF)
    for k, c in chunks(blocks):
        for r in rows:
            ds = dot(dh_ref[r, :], wdn[pl.ds(LANES * k, LANES * c), :], BY_T)
            for b in range(c):
                at = [pl.ds((2 * (k + b) + j) * LANES, LANES) for j in (0, 1)]
                s, dgate, dup = gated(gu0_ref[r, at[0]], gu0_ref[r, at[1]], ds[:, b * LANES : (b + 1) * LANES])
                s_ref[r, pl.ds((k + b) * LANES, LANES)] = s
                dgu0_ref[r, at[0]] = dgate
                dgu0_ref[r, at[1]] = dup
    acc[...] += dot(s_ref[...], dh_ref[...], T_BY)

    @pl.when(i == steps - 1)
    def _():
        dwd_ref[...] = acc[...].astype(BF)

    close()


def end_kernel(
    n, steps, todo, groups, count,
    a_ref, dgu_ref, d0_hbm, gu1, d1, wg, wu, wd, mg, mu, md, vg, vu, vd,
    out_g, out_u, out_d, mb_g, mb_u, mb_d, vb_g, vb_u, vb_d,
    all_g, all_u, all_d, own_gu, own_d, gbuf, dbuf, wb_g, wb_d, sq_send, sq_all, in_sem, sq_s, sq_r, ag_s, ag_r, put_sem, *ring_refs,
):
    i = pl.program_id(0)
    me = lax.axis_index("dp")
    d = md.shape[2]
    rg, rd = mg.shape[1], md.shape[1]
    my_g = pl.ds(pl.multiple_of(me * rg, rg), rg)
    my_d = pl.ds(pl.multiple_of(me * rd, rd), rd)
    width = dgu_ref.shape[1]
    rings = [Ring(n, own_d, *ring_refs[:3])]
    for k, (first, wide) in enumerate(groups):
        rings.append(Ring(n, own_gu.at[:, pl.ds(first * width, wide * width)], *ring_refs[3 * k + 3 : 3 * k + 6]))
    load = pltpu.make_async_copy(d0_hbm, own_d, in_sem.at[0])
    loads = [
        pltpu.make_async_copy(gu1, gbuf.at[1], in_sem.at[1]),
        pltpu.make_async_copy(d1, dbuf.at[1], in_sem.at[2]),
        pltpu.make_async_copy(mg, mb_g, in_sem.at[3]),
        pltpu.make_async_copy(mu, mb_u, in_sem.at[4]),
        pltpu.make_async_copy(md, mb_d, in_sem.at[5]),
        pltpu.make_async_copy(vg, vb_g, in_sem.at[6]),
        pltpu.make_async_copy(vu, vb_u, in_sem.at[7]),
        pltpu.make_async_copy(vd, vb_d, in_sem.at[8]),
        pltpu.make_async_copy(wg.at[:, my_g], wb_g.at[0], in_sem.at[9]),
        pltpu.make_async_copy(wu.at[:, my_g], wb_g.at[1], in_sem.at[10]),
        pltpu.make_async_copy(wd.at[:, my_d], wb_d, in_sem.at[11]),
    ]

    @pl.when(i == 0)
    def _():
        load.start()
        greet(n, tuple(range(1, n)))
        load.wait()
        rings[0].start()
        for c in loads:
            c.start()

    run_plan(todo, rings, steps)
    for k, (first, wide) in enumerate(groups):
        if first + wide < steps:

            @pl.when(i == first + wide)
            def _(k=k):
                rings[k + 1].start()

    own_gu[:, pl.ds(pl.multiple_of(i * width, width), width)] = dot(a_ref[...], dgu_ref[...], T_BY).astype(BF)

    @pl.when(i == steps - 1)
    def _():
        for c in loads:
            c.wait()
        for k, (first, wide) in enumerate(groups):
            if first + wide >= steps:
                rings[k + 1].start()
        rest_of_plan(todo, rings, steps)
        rings[0].finish(dbuf.at[0])
        for k, (first, wide) in enumerate(groups):
            rings[k + 1].finish(gbuf.at[0, :, pl.ds(first * width, wide * width)])

        def squares(t):
            t = t.astype(F32)
            t = t * t
            t = jnp.sum(t.reshape(t.shape[0] // 8, 8, t.shape[1]), 0)
            return sum(t[:, k : k + LANES] for k in range(0, t.shape[1], LANES))

        sq = squares(gbuf[0]) + squares(gbuf[1]) + squares(dbuf[0]) + squares(dbuf[1])
        sq_send[...] = sq
        to_all = [
            pltpu.make_async_remote_copy(
                src_ref=sq_send,
                dst_ref=sq_all.at[k - 1],
                send_sem=sq_s.at[k - 1],
                recv_sem=sq_r.at[k - 1],
                device_id={"dp": lax.rem(me + k, n)},
                device_id_type=MESH,
            )
            for k in range(1, n)
        ]
        for c in to_all:
            c.start()
        for c in to_all:
            c.wait_recv()
        total = jnp.sum(sq + jnp.sum(sq_all[...], 0), keepdims=True)
        factor = jnp.minimum(1.0, 0.5 * lax.rsqrt(total / count + 1e-30))

        streams = rings[0].streams

        def gathered(layer, down, half, owner, to=(all_g, all_u, all_d)):
            owner = lax.rem(owner + n, n)
            if down:
                return to[2].at[layer, pl.ds(pl.multiple_of(owner * rd, rd), rd), pl.ds(half * (d // 2), d // 2)]
            return to[half].at[layer, pl.ds(pl.multiple_of(owner * rg, rg), rg)]

        def put(layer, down, s, hop):
            half, way, _ = streams[s]
            where = layer, down, half, me - way * hop
            sem = put_sem.at[layer * 2 + down, s, hop]
            return pltpu.make_async_copy(gathered(*where), gathered(*where, (out_g, out_u, out_d)), sem)

        def copy(layer, down, s, hop, owner):
            part = gathered(layer, down, streams[s][0], owner)
            return pltpu.make_async_remote_copy(
                src_ref=part,
                dst_ref=part,
                send_sem=ag_s.at[layer * 2 + down, s, hop - 1],
                recv_sem=ag_r.at[layer * 2 + down, s, hop - 1],
                device_id={"dp": lax.rem(me + streams[s][1] + n, n)},
                device_id_type=MESH,
            )

        def sending(layer, down, s, hop):
            return copy(layer, down, s, hop, me - streams[s][1] * (hop - 1))

        def arrival(layer, down, s, hop):
            return copy(layer, down, s, hop, me - streams[s][1] * hop)

        def adamw(w_ref, m_ref, v_ref, g, out):
            g = g.astype(F32) * factor
            m = 0.9 * m_ref[...] + 0.1 * g
            v = 0.95 * v_ref[...] + 0.05 * g * g
            w = w_ref[...].astype(F32)
            out[...] = (w - 0.02 * (m * lax.rsqrt(v + 1e-8) + 0.1 * w)).astype(BF)
            m_ref[...] = m
            v_ref[...] = v

        units = [(layer, down) for layer in (0, 1) for down in (0, 1)]
        for layer, down in units:
            if down:
                adamw(wb_d.at[layer], mb_d.at[layer], vb_d.at[layer], dbuf[layer], all_d.at[layer, my_d])
            else:
                for j, (m, v, to) in enumerate(((mb_g, vb_g, all_g), (mb_u, vb_u, all_u))):
                    g = [gbuf[layer, :, k : k + LANES] for k in range(j * LANES, gbuf.shape[2], 2 * LANES)]
                    adamw(wb_g.at[j, layer], m.at[layer], v.at[layer], jnp.concatenate(g, 1), to.at[layer, my_g])
            for s in range(4):
                sending(layer, down, s, 1).start()
            for s in (0, 1):
                put(layer, down, s, 0).start()
        for hop in range(1, streams[0][2] + 1):
            for layer, down in units:
                for s in range(4):
                    if hop <= streams[s][2]:
                        arrival(layer, down, s, hop).wait_recv()
                        if hop < streams[s][2]:
                            sending(layer, down, s, hop + 1).start()
                        put(layer, down, s, hop).start()
        for c in to_all:
            c.wait_send()
        for layer, down in units:
            for s in range(4):
                for hop in range(1, streams[s][2] + 1):
                    sending(layer, down, s, hop).wait_send()
                for hop in range(0 if s < 2 else 1, streams[s][2] + 1):
                    put(layer, down, s, hop).wait()


def store_kernel(*refs):
    k = len(refs) // 2
    copies = [pltpu.make_async_copy(a, b, refs[-1].at[j]) for j, (a, b) in enumerate(zip(refs[:k], refs[k : 2 * k]))]
    for c in copies:
        c.start()
    for c in copies:
        c.wait()


def params(cid=None, mib=62):
    if cid is None:
        return pltpu.CompilerParams(vmem_limit_bytes=mib << 20)
    return pltpu.CompilerParams(vmem_limit_bytes=mib << 20, collective_id=cid, has_side_effects=True)


def solution(mesh):
    n = mesh.shape["dp"]
    hops = n // 2, n - 1 - n // 2

    def step(x, dy, wg, wu, wd, mg, mu, md, vg, vu, vd):
        x, dy = x[0], dy[0]
        tokens, d = x.shape
        ff = wd.shape[1]
        rg, rd = d // n, ff // n
        tile = 512
        steps = tokens // tile
        blocks = ff // LANES
        rows = lambda c: pl.BlockSpec((tile, c), lambda i: (i, 0))
        whole = lambda *s: pl.BlockSpec(s, lambda i: (0,) * len(s))
        once = lambda *s: pl.BlockSpec(s, lambda i: (0,) * len(s), pipeline_mode=pl.Buffered(1))
        columns = lambda r: pl.BlockSpec((r, 2 * LANES), lambda i: (0, i))
        array = jax.ShapeDtypeStruct
        sem, vm = pltpu.SemaphoreType.DMA, pltpu.VMEM
        mm = 2 * tokens * d * ff

        def us(row_count, cols):
            return row_count * cols * 2 / 46.6e3

        def ring(row_count, cols):
            return [vm((4, hops[0], row_count, cols // 2), BF), sem((4, hops[0])), sem((4, hops[0]))]

        gu0, h1, a0, a1, dgu1, dwd1 = pl.pallas_call(
            top_kernel,
            grid=(steps,),
            in_specs=[rows(d), rows(d), ANY, ANY, ANY],
            out_specs=[rows(2 * ff), rows(d), rows(d), rows(d), rows(2 * ff), whole(ff, d)],
            out_shape=[array((tokens, 2 * ff), F32)]
            + [array((tokens, d), BF)] * 3
            + [array((tokens, 2 * ff), BF), array((ff, d), BF)],
            scratch_shapes=[
                vm((2, d, 2 * ff), BF), vm((2, ff, d), BF), vm((tile, ff), BF), vm((ff, d), F32), sem((2, 2 * blocks)), sem((2,)),
            ],
            compiler_params=params(),
            cost_estimate=pl.CostEstimate(flops=7 * mm, bytes_accessed=90 << 20, transcendentals=0),
            name="top",
        )(x, dy, wg, wu, wd)

        dwgu1, sum_d1 = pl.pallas_call(
            functools.partial(gu_kernel, n, blocks, plan(hops, [(0, us(rd, d // 2))], blocks, 1.7)),
            grid=(blocks,),
            in_specs=[once(tokens, d), columns(tokens), ANY],
            out_specs=[columns(d), whole(rd, d)],
            out_shape=[array((d, 2 * ff), BF), array((rd, d), BF)],
            scratch_shapes=[vm((ff, d), BF), sem(())] + ring(rd, d),
            compiler_params=params(0),
            cost_estimate=pl.CostEstimate(flops=2 * mm, bytes_accessed=30 << 20, transcendentals=0),
            name="gu1",
        )(a1, dgu1, dwd1)

        dgu0, dwd0, sum_gu1 = pl.pallas_call(
            functools.partial(mid_kernel, n, steps, plan(hops, [(0, us(rg, ff))], steps, 6.0)),
            grid=(steps,),
            in_specs=[rows(d), rows(d), rows(2 * ff), rows(2 * ff), ANY, ANY, ANY, ANY],
            out_specs=[rows(2 * ff), whole(ff, d), whole(rg, 2 * ff)],
            out_shape=[array((tokens, 2 * ff), BF), array((ff, d), BF), array((rg, 2 * ff), BF)],
            scratch_shapes=[
                vm((d, 2 * ff), BF), vm((ff, d), BF), vm((tile, ff), BF), vm((tile, d), BF), vm((ff, d), F32),
                sem((2 * blocks,)), sem(()), vm((d, 2 * ff), BF), sem(()),
            ] + ring(rg, 2 * ff),
            compiler_params=params(1),
            cost_estimate=pl.CostEstimate(flops=4 * mm, bytes_accessed=100 << 20, transcendentals=0),
            name="mid",
        )(h1, dy, dgu1, gu0, wg, wu, wd, dwgu1)

        groups, first = [], 0
        for k in range(3):
            wide = -(-(blocks - first) // (3 - k))
            groups.append((first, wide))
            first += wide
        todo = plan(hops, [(0, us(rd, d // 2))] + [(f + w, us(rg, w * LANES)) for f, w in groups], blocks, 1.7)
        outs = pl.pallas_call(
            functools.partial(end_kernel, n, blocks, todo, groups, float(wg.size + wu.size + wd.size)),
            grid=(blocks,),
            in_specs=[once(tokens, d), columns(tokens)] + [ANY] * 12,
            out_specs=[pl.BlockSpec(memory_space=pltpu.VMEM)] * 9,
            out_shape=[vm(t.shape, BF) for t in (wg, wu, wd)] + [vm(t.shape, F32) for t in (mg, mu, md, vg, vu, vd)],
            scratch_shapes=[
                vm(wg.shape, BF), vm(wu.shape, BF), vm(wd.shape, BF),
                vm((d, 2 * ff), BF), vm((ff, d), BF), vm((2, rg, 2 * ff), BF), vm((2, rd, d), BF),
                vm((2, *mg.shape), BF), vm(md.shape, BF), vm((8, LANES), F32), vm((n - 1, 8, LANES), F32),
                sem((12,)), sem((n - 1,)), sem((n - 1,)), sem((4, 4, hops[0])), sem((4, 4, hops[0])), sem((4, 4, hops[0] + 1)),
            ] + ring(rd, d) + [r for _, w in groups for r in ring(rg, w * 2 * LANES)],
            compiler_params=params(2, 40),
            cost_estimate=pl.CostEstimate(flops=2 * mm, bytes_accessed=30 << 20, transcendentals=0),
            name="end",
        )(a0, dgu0, dwd0, sum_gu1, sum_d1, wg, wu, wd, mg, mu, md, vg, vu, vd)
        return tuple(
            pl.pallas_call(
                store_kernel,
                in_specs=[pl.BlockSpec(memory_space=pltpu.VMEM)] * 9,
                out_specs=[ANY] * 9,
                out_shape=[array(t.shape, t.dtype) for t in outs],
                scratch_shapes=[sem((9,))],
                compiler_params=params(None, 2),
                name="store",
            )(*outs)
        )

    seq, whole, rows = P(("rep", "dp"), None, None), P(None, None, None), P(None, "dp", None)
    return jax.shard_map(
        step,
        mesh=mesh,
        in_specs=(seq, seq) + (whole,) * 3 + (rows,) * 6,
        out_specs=(P("rep", None, None),) * 3 + (P("rep", "dp", None),) * 6,
        check_vma=False,
    )
```

```python
import functools

import jax
import jax.numpy as jnp
from jax import lax
from jax.experimental import pallas as pl
from jax.experimental.pallas import tpu as pltpu
from jax.sharding import PartitionSpec as P

BF, F32 = jnp.bfloat16, jnp.float32
MESH = pl.DeviceIdType.MESH
ANY = pl.BlockSpec(memory_space=pl.ANY)
ROWS = (((1,), (0,)), ((), ()))
BY_T = (((1,), (1,)), ((), ()))
T_BY = (((0,), (0,)), ((), ()))


def dot(a, b, dims):
    return lax.dot_general(a, b, dims, preferred_element_type=F32)


def rms_scale(wide):
    return lax.rsqrt(jnp.mean(wide * wide, -1, keepdims=True) + 1e-6)


def sigmoid(t):
    return 1.0 / (1.0 + jnp.exp(-t))


class Ring:
    def __init__(self, n, own, recv, send_sem, recv_sem):
        self.n, self.own, self.recv, self.send_sem, self.recv_sem = n, own, recv, send_sem, recv_sem
        self.rows, self.half = recv.shape[2], recv.shape[3]
        far, near = n // 2, n - 1 - n // 2
        self.streams = ((0, 1, far), (1, -1, far), (1, 1, near), (0, -1, near))
        self.me = lax.axis_index("dp")

    def mine(self, owner, half):
        owner = lax.rem(owner + self.n, self.n)
        rows = pl.ds(pl.multiple_of(owner * self.rows, self.rows), self.rows)
        return self.own.at[rows, pl.ds(half * self.half, self.half)]

    def copy(self, s, hop):
        half, way, hops = self.streams[s]
        src = self.mine(self.me + way * hops, half) if hop == 1 else self.recv.at[s, hop - 2]
        to = lax.rem(self.me + way + self.n, self.n)
        return pltpu.make_async_remote_copy(
            src_ref=src,
            dst_ref=self.recv.at[s, hop - 1],
            send_sem=self.send_sem.at[s, hop - 1],
            recv_sem=self.recv_sem.at[s, hop - 1],
            device_id={"dp": to},
            device_id_type=MESH,
        )

    def start(self):
        for s in range(4):
            self.copy(s, 1).start()

    def add(self, s, hop):
        half, way, hops = self.streams[s]
        self.copy(s, hop).wait_recv()
        if hop < hops:
            buf = self.recv.at[s, hop - 1]
            term = self.mine(self.me + way * (hops - hop), half)
            buf[...] = (buf[...].astype(F32) + term[...].astype(F32)).astype(BF)

    def send(self, s, hop):
        if hop < self.streams[s][2]:
            self.copy(s, hop + 1).start()

    def handle(self, pair):
        for s, hop in pair:
            self.add(s, hop)
        for s, hop in pair:
            self.send(s, hop)

    def finish(self, out):
        for half in (0, 1):
            total = self.mine(self.me, half)[...].astype(F32)
            for s, (its, _, hops) in enumerate(self.streams):
                if its == half:
                    total = total + self.recv[s, hops - 1].astype(F32)
            out[:, pl.ds(half * self.half, self.half)] = total.astype(BF)
        for s, (_, _, hops) in enumerate(self.streams):
            for hop in range(1, hops + 1):
                self.copy(s, hop).wait_send()


def greet(n, others):
    me = lax.axis_index("dp")
    barrier = pltpu.get_barrier_semaphore()
    for d in others:
        pl.semaphore_signal(barrier, inc=1, device_id={"dp": lax.rem(me + d + n, n)}, device_id_type=MESH)
    pl.semaphore_wait(barrier, len(others))


def plan(hops, rings, steps, step_us):
    latency, free, waiting, out = 2.5, 0.0, [], []
    far, near = hops

    def send(ring, group, hop, now):
        nonlocal free
        free = max(free, now) + rings[ring][1]
        waiting.append((free + latency, ring, group, hop))

    step, now = 0, 0.0
    while step < steps or waiting:
        if step < steps:
            now = step * step_us
        else:
            now = max(steps * step_us, min(w[0] for w in waiting))
        for w in sorted(w for w in waiting if w[0] <= now):
            waiting.remove(w)
            _, ring, group, hop = w
            out.append((min(step, steps), ring, tuple((s, hop) for s in ((0, 1), (2, 3))[group])))
            if hop < (far, near)[group]:
                send(ring, group, hop + 1, now)
        for ring, (start, _) in enumerate(rings):
            if start == step:
                send(ring, 0, 1, now)
                send(ring, 1, 1, now)
        step += 1
    return out


def run_plan(todo, rings, steps):
    i = pl.program_id(0)
    for step in range(1, steps):
        now = [(r, pair) for at, r, pair in todo if at == step]
        if now:

            @pl.when(i == step)
            def _(now=now):
                for r, pair in now:
                    rings[r].handle(pair)


def rest_of_plan(todo, rings, steps):
    for at, r, pair in todo:
        if at >= steps:
            rings[r].handle(pair)


def with_ring(n, steps, todo, refs, own_hbm, out):
    own, load_sem, recv, send_sem, recv_sem = refs
    i = pl.program_id(0)
    ring = Ring(n, own, recv, send_sem, recv_sem)
    load = pltpu.make_async_copy(own_hbm, own, load_sem)

    @pl.when(i == 0)
    def _():
        load.start()
        greet(n, (1, -1))
        load.wait()
        ring.start()

    run_plan(todo, [ring], steps)

    def close():
        @pl.when(i == steps - 1)
        def _():
            rest_of_plan(todo, [ring], steps)
            ring.finish(out)

    return close


def load_all(copies):
    @pl.when(pl.program_id(0) == 0)
    def _():
        for c in copies:
            c.start()
        for c in copies:
            c.wait()


LANES = 128


def gate_up_copies(wg, wu, wgu, sem, blocks):
    out = []
    for k in range(blocks):
        for j, w in enumerate((wg, wu)):
            to = wgu.at[:, pl.ds(LANES * (2 * k + j), LANES)]
            out.append(pltpu.make_async_copy(w.at[:, pl.ds(LANES * k, LANES)], to, sem.at[2 * k + j]))
    return out


def chunks(blocks):
    return [(k, min(2, blocks - k)) for k in range(0, blocks, 2)]


def halves(ref):
    rows = ref.shape[0] // 2
    return [pl.ds(0, rows), pl.ds(rows, rows)]


def gated(gate, up, ds):
    sig = sigmoid(gate)
    silu = gate * sig
    ds = ds.astype(BF).astype(F32)
    return (ds * up * (sig + silu * (1.0 - sig))).astype(BF), (ds * silu).astype(BF)


def top_kernel(x_ref, dy_ref, wg, wu, wd, gu0_ref, gu1_ref, s0_ref, h1_ref, a0_ref, a1_ref, dwd_ref, wgu, wdn, s_ref, acc, sem, dsem):
    i = pl.program_id(0)
    blocks = wd.shape[1] // LANES
    load_all(
        [c for k in (0, 1) for c in gate_up_copies(wg.at[k], wu.at[k], wgu.at[k], sem.at[k], blocks)]
        + [pltpu.make_async_copy(wd.at[0], wdn, dsem)]
    )

    @pl.when(i == 0)
    def _():
        acc[...] = jnp.zeros_like(acc)

    rows = halves(x_ref)

    def gate_up(layer, a_ref, gu_ref, to):
        for k, c in chunks(blocks):
            at = pl.ds(2 * LANES * k, 2 * LANES * c)
            for r in rows:
                gu = dot(a_ref[r, :], wgu[layer, :, at], ROWS)
                gu_ref[r, at] = gu
                for b in range(c):
                    gate, up = (gu[:, (2 * b + j) * LANES : (2 * b + j + 1) * LANES] for j in (0, 1))
                    to[r, pl.ds((k + b) * LANES, LANES)] = (gate * sigmoid(gate) * up).astype(BF)

    for r in rows:
        x = x_ref[r, :].astype(F32)
        a0_ref[r, :] = (x * rms_scale(x)).astype(BF)
    gate_up(0, a0_ref, gu0_ref, s0_ref)
    for r in rows:
        h = x_ref[r, :].astype(F32) + dot(s0_ref[r, :], wdn[...], ROWS).astype(BF).astype(F32)
        h = h.astype(BF)
        h1_ref[r, :] = h
        h = h.astype(F32)
        a1_ref[r, :] = (h * rms_scale(h)).astype(BF)
    gate_up(1, a1_ref, gu1_ref, s_ref)
    acc[...] += dot(s_ref[...], dy_ref[...], T_BY)

    @pl.when(i == pl.num_programs(0) - 1)
    def _():
        dwd_ref[...] = acc[...].astype(BF)


def back_of_chunk(dh_ref, a_ref, gu_ref, wd_ref, dgu_ref, blocks, keep):
    i = pl.program_id(0)
    tokens = gu_ref.shape[0]
    part = tokens // 4

    def run(c, half):
        for k in range(4):
            r = pl.ds(k * part, part)
            everywhere = pl.ds(half * tokens + k * part, part)
            ds = dot(dh_ref[everywhere, :], wd_ref[0, pl.ds(0, c * LANES), :], BY_T)
            for b in range(c):
                at = [pl.ds((2 * b + j) * LANES, LANES) for j in (0, 1)]
                dgate, dup = gated(gu_ref[r, at[0]], gu_ref[r, at[1]], ds[:, b * LANES : (b + 1) * LANES])
                dgu_ref[everywhere, at[0]] = dgate
                dgu_ref[everywhere, at[1]] = dup
        if half == 1:
            wide = 2 * c * LANES
            keep(i // 2, wide, dot(a_ref[...], dgu_ref[:, pl.ds(0, wide)], T_BY).astype(BF))

    whole_chunks = blocks // 2
    for half in (0, 1):

        @pl.when((i < 2 * whole_chunks) & (lax.rem(i, 2) == half))
        def _(half=half):
            run(2, half)

        if blocks % 2:

            @pl.when(i == 2 * whole_chunks + half)
            def _(half=half):
                run(1, half)


def back_kernel(n, steps, todo, blocks, dh_ref, a_ref, gu_ref, wd_ref, own_hbm, dgu_ref, dw_ref, sum_ref, *ring):
    close = with_ring(n, steps, todo, ring, own_hbm, sum_ref)

    def keep(chunk, wide, dw):
        dw_ref[:, pl.ds(0, wide)] = dw

    back_of_chunk(dh_ref, a_ref, gu_ref, wd_ref, dgu_ref, blocks, keep)
    close()


def mid_kernel(
    n, steps, todo, h1_ref, dy_ref, dgu1_ref, s0_ref, wg, wu, own_hbm, dh_ref, dwd_ref, sum_ref, wgu, acc, sem, *ring,
):
    i = pl.program_id(0)
    close = with_ring(n, steps, todo, ring, own_hbm, sum_ref)
    load_all(gate_up_copies(wg.at[1], wu.at[1], wgu, sem, wg.shape[2] // LANES))

    @pl.when(i == 0)
    def _():
        acc[...] = jnp.zeros_like(acc)

    for r in halves(h1_ref):
        da = dot(dgu1_ref[r, :], wgu[...], BY_T).astype(BF).astype(F32)
        h = h1_ref[r, :].astype(F32)
        scale = rms_scale(h)
        back = scale * (da - h * (scale * scale * jnp.mean(da * h, -1, keepdims=True)))
        dh_ref[r, :] = (dy_ref[r, :].astype(F32) + back.astype(BF).astype(F32)).astype(BF)
    acc[...] += dot(s0_ref[...], dh_ref[...], T_BY)

    @pl.when(i == steps - 1)
    def _():
        dwd_ref[...] = acc[...].astype(BF)

    close()


def end_kernel(
    n, steps, todo, groups, count,
    dh_ref, a_ref, gu_ref, wd_ref, d0_hbm, gu1, d1, wg, wu, wd, mg, mu, md, vg, vu, vd,
    out_g, out_u, out_d, mb_g, mb_u, mb_d, vb_g, vb_u, vb_d,
    dgu_ref, all_g, all_u, all_d, own_gu, own_d, gbuf, dbuf, wb_g, wb_d, sq_send, sq_all, in_sem, sq_s, sq_r, ag_s, ag_r, put_sem, *ring_refs,
):
    i = pl.program_id(0)
    me = lax.axis_index("dp")
    d = md.shape[2]
    rg, rd = mg.shape[1], md.shape[1]
    my_g = pl.ds(pl.multiple_of(me * rg, rg), rg)
    my_d = pl.ds(pl.multiple_of(me * rd, rd), rd)
    width = gu_ref.shape[1]
    blocks = wg.shape[2] // LANES
    rings = [Ring(n, own_d, *ring_refs[:3])]
    for k, ((first, wide), _) in enumerate(groups):
        rings.append(Ring(n, own_gu.at[:, pl.ds(first * 2 * LANES, wide * 2 * LANES)], *ring_refs[3 * k + 3 : 3 * k + 6]))
    load = pltpu.make_async_copy(d0_hbm, own_d, in_sem.at[0])
    loads = [
        pltpu.make_async_copy(gu1, gbuf.at[1], in_sem.at[1]),
        pltpu.make_async_copy(d1, dbuf.at[1], in_sem.at[2]),
        pltpu.make_async_copy(mg, mb_g, in_sem.at[3]),
        pltpu.make_async_copy(mu, mb_u, in_sem.at[4]),
        pltpu.make_async_copy(md, mb_d, in_sem.at[5]),
        pltpu.make_async_copy(vg, vb_g, in_sem.at[6]),
        pltpu.make_async_copy(vu, vb_u, in_sem.at[7]),
        pltpu.make_async_copy(vd, vb_d, in_sem.at[8]),
        pltpu.make_async_copy(wg.at[:, my_g], wb_g.at[0], in_sem.at[9]),
        pltpu.make_async_copy(wu.at[:, my_g], wb_g.at[1], in_sem.at[10]),
        pltpu.make_async_copy(wd.at[:, my_d], wb_d, in_sem.at[11]),
    ]

    @pl.when(i == 0)
    def _():
        load.start()
        greet(n, tuple(range(1, n)))
        load.wait()
        rings[0].start()
        for c in loads:
            c.start()

    run_plan(todo, rings, steps)
    for k, (_, at) in enumerate(groups):
        if at < steps:

            @pl.when(i == at)
            def _(k=k):
                rings[k + 1].start()

    def keep(chunk, wide, dw):
        own_gu[:, pl.ds(pl.multiple_of(chunk * width, width), wide)] = dw

    back_of_chunk(dh_ref, a_ref, gu_ref, wd_ref, dgu_ref, blocks, keep)

    @pl.when(i == steps - 1)
    def _():
        for c in loads:
            c.wait()
        for k, (_, at) in enumerate(groups):
            if at >= steps:
                rings[k + 1].start()
        rest_of_plan(todo, rings, steps)
        rings[0].finish(dbuf.at[0])
        for k, ((first, wide), _) in enumerate(groups):
            rings[k + 1].finish(gbuf.at[0, :, pl.ds(first * 2 * LANES, wide * 2 * LANES)])

        def squares(t):
            t = t.astype(F32)
            t = t * t
            t = jnp.sum(t.reshape(t.shape[0] // 8, 8, t.shape[1]), 0)
            return sum(t[:, k : k + LANES] for k in range(0, t.shape[1], LANES))

        sq = squares(gbuf[0]) + squares(gbuf[1]) + squares(dbuf[0]) + squares(dbuf[1])
        sq_send[...] = sq
        to_all = [
            pltpu.make_async_remote_copy(
                src_ref=sq_send,
                dst_ref=sq_all.at[k - 1],
                send_sem=sq_s.at[k - 1],
                recv_sem=sq_r.at[k - 1],
                device_id={"dp": lax.rem(me + k, n)},
                device_id_type=MESH,
            )
            for k in range(1, n)
        ]
        for c in to_all:
            c.start()
        for c in to_all:
            c.wait_recv()
        total = jnp.sum(sq + jnp.sum(sq_all[...], 0), keepdims=True)
        factor = jnp.minimum(1.0, 0.5 * lax.rsqrt(total / count + 1e-30))

        streams = rings[0].streams

        def gathered(layer, down, half, owner, to=(all_g, all_u, all_d)):
            owner = lax.rem(owner + n, n)
            if down:
                return to[2].at[layer, pl.ds(pl.multiple_of(owner * rd, rd), rd), pl.ds(half * (d // 2), d // 2)]
            return to[half].at[layer, pl.ds(pl.multiple_of(owner * rg, rg), rg)]

        def put(layer, down, s, hop):
            half, way, _ = streams[s]
            where = layer, down, half, me - way * hop
            sem = put_sem.at[layer * 2 + down, s, hop]
            return pltpu.make_async_copy(gathered(*where), gathered(*where, (out_g, out_u, out_d)), sem)

        def copy(layer, down, s, hop, owner):
            part = gathered(layer, down, streams[s][0], owner)
            return pltpu.make_async_remote_copy(
                src_ref=part,
                dst_ref=part,
                send_sem=ag_s.at[layer * 2 + down, s, hop - 1],
                recv_sem=ag_r.at[layer * 2 + down, s, hop - 1],
                device_id={"dp": lax.rem(me + streams[s][1] + n, n)},
                device_id_type=MESH,
            )

        def sending(layer, down, s, hop):
            return copy(layer, down, s, hop, me - streams[s][1] * (hop - 1))

        def arrival(layer, down, s, hop):
            return copy(layer, down, s, hop, me - streams[s][1] * hop)

        def adamw(w_ref, m_ref, v_ref, g, out):
            g = g.astype(F32) * factor
            m = 0.9 * m_ref[...] + 0.1 * g
            v = 0.95 * v_ref[...] + 0.05 * g * g
            w = w_ref[...].astype(F32)
            out[...] = (w - 0.02 * (m * lax.rsqrt(v + 1e-8) + 0.1 * w)).astype(BF)
            m_ref[...] = m
            v_ref[...] = v

        units = [(layer, down) for layer in (0, 1) for down in (0, 1)]
        for layer, down in units:
            if down:
                adamw(wb_d.at[layer], mb_d.at[layer], vb_d.at[layer], dbuf[layer], all_d.at[layer, my_d])
            else:
                for j, (m, v, to) in enumerate(((mb_g, vb_g, all_g), (mb_u, vb_u, all_u))):
                    g = [gbuf[layer, :, k : k + LANES] for k in range(j * LANES, gbuf.shape[2], 2 * LANES)]
                    adamw(wb_g.at[j, layer], m.at[layer], v.at[layer], jnp.concatenate(g, 1), to.at[layer, my_g])
            for s in range(4):
                sending(layer, down, s, 1).start()
            for s in (0, 1):
                put(layer, down, s, 0).start()
        for hop in range(1, streams[0][2] + 1):
            for layer, down in units:
                for s in range(4):
                    if hop <= streams[s][2]:
                        arrival(layer, down, s, hop).wait_recv()
                        if hop < streams[s][2]:
                            sending(layer, down, s, hop + 1).start()
                        put(layer, down, s, hop).start()
        for c in to_all:
            c.wait_send()
        for layer, down in units:
            for s in range(4):
                for hop in range(1, streams[s][2] + 1):
                    sending(layer, down, s, hop).wait_send()
                for hop in range(0 if s < 2 else 1, streams[s][2] + 1):
                    put(layer, down, s, hop).wait()


def store_kernel(*refs):
    k = len(refs) // 2
    copies = [pltpu.make_async_copy(a, b, refs[-1].at[j]) for j, (a, b) in enumerate(zip(refs[:k], refs[k : 2 * k]))]
    for c in copies:
        c.start()
    for c in copies:
        c.wait()


def params(cid=None, mib=62):
    if cid is None:
        return pltpu.CompilerParams(vmem_limit_bytes=mib << 20)
    return pltpu.CompilerParams(vmem_limit_bytes=mib << 20, collective_id=cid, has_side_effects=True)


def solution(mesh):
    n = mesh.shape["dp"]
    hops = n // 2, n - 1 - n // 2

    def step(x, dy, wg, wu, wd, mg, mu, md, vg, vu, vd):
        x, dy = x[0], dy[0]
        tokens, d = x.shape
        ff = wd.shape[1]
        rg, rd = d // n, ff // n
        tile = 512
        steps = tokens // tile
        blocks = ff // LANES
        rows = lambda c: pl.BlockSpec((tile, c), lambda i: (i, 0))
        whole = lambda *s: pl.BlockSpec(s, lambda i: (0,) * len(s))
        once = lambda *s: pl.BlockSpec(s, lambda i: (0,) * len(s), pipeline_mode=pl.Buffered(1))
        array = jax.ShapeDtypeStruct
        sem, vm = pltpu.SemaphoreType.DMA, pltpu.VMEM
        mm = 2 * tokens * d * ff

        def us(row_count, cols):
            return row_count * cols * 2 / 46.6e3

        def ring(row_count, cols):
            return [vm((4, hops[0], row_count, cols // 2), BF), sem((4, hops[0])), sem((4, hops[0]))]

        gu0, gu1, s0, h1, a0, a1, dwd1 = pl.pallas_call(
            top_kernel,
            grid=(steps,),
            in_specs=[rows(d), rows(d), ANY, ANY, ANY],
            out_specs=[rows(2 * ff), rows(2 * ff), rows(ff), rows(d), rows(d), rows(d), whole(ff, d)],
            out_shape=[array((tokens, 2 * ff), F32)] * 2
            + [array((tokens, ff), BF)]
            + [array((tokens, d), BF)] * 3
            + [array((ff, d), BF)],
            scratch_shapes=[
                vm((2, d, 2 * ff), BF), vm((ff, d), BF), vm((tile, ff), BF), vm((ff, d), F32), sem((2, 2 * blocks)), sem(()),
            ],
            compiler_params=params(),
            cost_estimate=pl.CostEstimate(flops=6 * mm, bytes_accessed=130 << 20, transcendentals=0),
            name="top",
        )(x, dy, wg, wu, wd)

        pieces = 2 * -(-blocks // 2)
        of_chunk = lambda layer: [
            once(tokens, d),
            once(tokens, d),
            pl.BlockSpec((tokens // 2, 4 * LANES), lambda i: (lax.rem(i, 2), i // 2)),
            pl.BlockSpec((1, 2 * LANES, d), lambda i: (layer, i // 2, 0)),
        ]
        columns = lambda r: pl.BlockSpec((r, 4 * LANES), lambda i: (0, i // 2))
        dgu1, dwgu1, sum_d1 = pl.pallas_call(
            functools.partial(back_kernel, n, pieces, plan(hops, [(0, us(rd, d // 2))], pieces, 2.2), blocks),
            grid=(pieces,),
            in_specs=of_chunk(1) + [ANY],
            out_specs=[columns(tokens), columns(d), whole(rd, d)],
            out_shape=[array((tokens, 2 * ff), BF), array((d, 2 * ff), BF), array((rd, d), BF)],
            scratch_shapes=[vm((ff, d), BF), sem(())] + ring(rd, d),
            compiler_params=params(0),
            cost_estimate=pl.CostEstimate(flops=3 * mm, bytes_accessed=80 << 20, transcendentals=0),
            name="back1",
        )(dy, a1, gu1, wd, dwd1)

        dh1, dwd0, sum_gu1 = pl.pallas_call(
            functools.partial(mid_kernel, n, steps, plan(hops, [(0, us(rg, ff))], steps, 3.5)),
            grid=(steps,),
            in_specs=[rows(d), rows(d), rows(2 * ff), rows(ff), ANY, ANY, ANY],
            out_specs=[rows(d), whole(ff, d), whole(rg, 2 * ff)],
            out_shape=[array((tokens, d), BF), array((ff, d), BF), array((rg, 2 * ff), BF)],
            scratch_shapes=[vm((d, 2 * ff), BF), vm((ff, d), F32), sem((2 * blocks,)), vm((d, 2 * ff), BF), sem(())]
            + ring(rg, 2 * ff),
            compiler_params=params(1),
            cost_estimate=pl.CostEstimate(flops=3 * mm, bytes_accessed=50 << 20, transcendentals=0),
            name="mid",
        )(h1, dy, dgu1, s0, wg, wu, dwgu1)

        groups = [(k, min(4, blocks - k)) for k in range(0, blocks, 4)]
        ready = [min(2 * -(-(f + w) // 2), pieces) for f, w in groups]
        todo = plan(hops, [(0, us(rd, d // 2))] + [(at, us(rg, w * LANES)) for at, (_, w) in zip(ready, groups)], pieces, 2.2)
        outs = pl.pallas_call(
            functools.partial(end_kernel, n, pieces, todo, list(zip(groups, ready)), float(wg.size + wu.size + wd.size)),
            grid=(pieces,),
            in_specs=of_chunk(0) + [ANY] * 12,
            out_specs=[pl.BlockSpec(memory_space=pltpu.VMEM)] * 9,
            out_shape=[vm(t.shape, BF) for t in (wg, wu, wd)] + [vm(t.shape, F32) for t in (mg, mu, md, vg, vu, vd)],
            scratch_shapes=[
                vm((tokens, 4 * LANES), BF), vm(wg.shape, BF), vm(wu.shape, BF), vm(wd.shape, BF),
                vm((d, 2 * ff), BF), vm((ff, d), BF), vm((2, rg, 2 * ff), BF), vm((2, rd, d), BF),
                vm((2, *mg.shape), BF), vm(md.shape, BF), vm((8, LANES), F32), vm((n - 1, 8, LANES), F32),
                sem((12,)), sem((n - 1,)), sem((n - 1,)), sem((4, 4, hops[0])), sem((4, 4, hops[0])), sem((4, 4, hops[0] + 1)),
            ] + ring(rd, d) + [r for _, w in groups for r in ring(rg, w * 2 * LANES)],
            compiler_params=params(2, 48),
            cost_estimate=pl.CostEstimate(flops=2 * mm, bytes_accessed=30 << 20, transcendentals=0),
            name="end",
        )(dh1, a0, gu0, wd, dwd0, sum_gu1, sum_d1, wg, wu, wd, mg, mu, md, vg, vu, vd)
        return tuple(
            pl.pallas_call(
                store_kernel,
                in_specs=[pl.BlockSpec(memory_space=pltpu.VMEM)] * 9,
                out_specs=[ANY] * 9,
                out_shape=[array(t.shape, t.dtype) for t in outs],
                scratch_shapes=[sem((9,))],
                compiler_params=params(None, 2),
                name="store",
            )(*outs)
        )

    seq, whole, rows = P(("rep", "dp"), None, None), P(None, None, None), P(None, "dp", None)
    return jax.shard_map(
        step,
        mesh=mesh,
        in_specs=(seq, seq) + (whole,) * 3 + (rows,) * 6,
        out_specs=(P("rep", None, None),) * 3 + (P("rep", "dp", None),) * 6,
        check_vma=False,
    )
```

```python
import functools

import jax
import jax.numpy as jnp
from jax import lax
from jax.experimental import pallas as pl
from jax.experimental.pallas import tpu as pltpu
from jax.sharding import PartitionSpec as P

BF, F32 = jnp.bfloat16, jnp.float32
MESH = pl.DeviceIdType.MESH
ANY = pl.BlockSpec(memory_space=pl.ANY)
ROWS = (((1,), (0,)), ((), ()))
BY_T = (((1,), (1,)), ((), ()))
T_BY = (((0,), (0,)), ((), ()))


def dot(a, b, dims):
    return lax.dot_general(a, b, dims, preferred_element_type=F32)


def rms_scale(wide):
    return lax.rsqrt(jnp.mean(wide * wide, -1, keepdims=True) + 1e-6)


def sigmoid(t):
    return 1.0 / (1.0 + jnp.exp(-t))


class Ring:
    def __init__(self, n, own, recv, send_sem, recv_sem):
        self.n, self.own, self.recv, self.send_sem, self.recv_sem = n, own, recv, send_sem, recv_sem
        self.rows, self.half = recv.shape[2], recv.shape[3]
        far, near = n // 2, n - 1 - n // 2
        self.streams = ((0, 1, far), (1, -1, far), (1, 1, near), (0, -1, near))
        self.me = lax.axis_index("dp")

    def mine(self, owner, half):
        owner = lax.rem(owner + self.n, self.n)
        rows = pl.ds(pl.multiple_of(owner * self.rows, self.rows), self.rows)
        return self.own.at[rows, pl.ds(half * self.half, self.half)]

    def copy(self, s, hop):
        half, way, hops = self.streams[s]
        src = self.mine(self.me + way * hops, half) if hop == 1 else self.recv.at[s, hop - 2]
        to = lax.rem(self.me + way + self.n, self.n)
        return pltpu.make_async_remote_copy(
            src_ref=src,
            dst_ref=self.recv.at[s, hop - 1],
            send_sem=self.send_sem.at[s, hop - 1],
            recv_sem=self.recv_sem.at[s, hop - 1],
            device_id={"dp": to},
            device_id_type=MESH,
        )

    def start(self):
        for s in range(4):
            self.copy(s, 1).start()

    def add(self, s, hop):
        half, way, hops = self.streams[s]
        self.copy(s, hop).wait_recv()
        if hop < hops:
            buf = self.recv.at[s, hop - 1]
            term = self.mine(self.me + way * (hops - hop), half)
            buf[...] = (buf[...].astype(F32) + term[...].astype(F32)).astype(BF)

    def send(self, s, hop):
        if hop < self.streams[s][2]:
            self.copy(s, hop + 1).start()

    def handle(self, pair):
        for s, hop in pair:
            self.add(s, hop)
        for s, hop in pair:
            self.send(s, hop)

    def finish(self, out):
        for half in (0, 1):
            total = self.mine(self.me, half)[...].astype(F32)
            for s, (its, _, hops) in enumerate(self.streams):
                if its == half:
                    total = total + self.recv[s, hops - 1].astype(F32)
            out[:, pl.ds(half * self.half, self.half)] = total.astype(BF)
        for s, (_, _, hops) in enumerate(self.streams):
            for hop in range(1, hops + 1):
                self.copy(s, hop).wait_send()


def greet(n, others):
    me = lax.axis_index("dp")
    barrier = pltpu.get_barrier_semaphore()
    for d in others:
        pl.semaphore_signal(barrier, inc=1, device_id={"dp": lax.rem(me + d + n, n)}, device_id_type=MESH)
    pl.semaphore_wait(barrier, len(others))


def plan(hops, rings, steps, step_us):
    latency, free, waiting, out = 2.5, 0.0, [], []
    far, near = hops

    def send(ring, group, hop, now):
        nonlocal free
        free = max(free, now) + rings[ring][1]
        waiting.append((free + latency, ring, group, hop))

    step, now = 0, 0.0
    while step < steps or waiting:
        if step < steps:
            now = step * step_us
        else:
            now = max(steps * step_us, min(w[0] for w in waiting))
        for w in sorted(w for w in waiting if w[0] <= now):
            waiting.remove(w)
            _, ring, group, hop = w
            out.append((min(step, steps), ring, tuple((s, hop) for s in ((0, 1), (2, 3))[group])))
            if hop < (far, near)[group]:
                send(ring, group, hop + 1, now)
        for ring, (start, _) in enumerate(rings):
            if start == step:
                send(ring, 0, 1, now)
                send(ring, 1, 1, now)
        step += 1
    return out


def run_plan(todo, rings, steps):
    i = pl.program_id(0)
    for step in range(1, steps):
        now = [(r, pair) for at, r, pair in todo if at == step]
        if now:

            @pl.when(i == step)
            def _(now=now):
                for r, pair in now:
                    rings[r].handle(pair)


def rest_of_plan(todo, rings, steps):
    for at, r, pair in todo:
        if at >= steps:
            rings[r].handle(pair)


def with_ring(n, steps, todo, refs, own_hbm, out):
    own, load_sem, recv, send_sem, recv_sem = refs
    i = pl.program_id(0)
    ring = Ring(n, own, recv, send_sem, recv_sem)
    load = pltpu.make_async_copy(own_hbm, own, load_sem)

    @pl.when(i == 0)
    def _():
        load.start()
        greet(n, (1, -1))
        load.wait()
        ring.start()

    run_plan(todo, [ring], steps)

    def close():
        @pl.when(i == steps - 1)
        def _():
            rest_of_plan(todo, [ring], steps)
            ring.finish(out)

    return close


def load_all(copies):
    @pl.when(pl.program_id(0) == 0)
    def _():
        for c in copies:
            c.start()
        for c in copies:
            c.wait()


LANES = 128


def gate_up_copies(wg, wu, wgu, sem, blocks):
    out = []
    for k in range(blocks):
        for j, w in enumerate((wg, wu)):
            to = wgu.at[:, pl.ds(LANES * (2 * k + j), LANES)]
            out.append(pltpu.make_async_copy(w.at[:, pl.ds(LANES * k, LANES)], to, sem.at[2 * k + j]))
    return out


def chunks(blocks):
    return [(k, min(2, blocks - k)) for k in range(0, blocks, 2)]


def halves(ref):
    rows = ref.shape[0] // 2
    return [pl.ds(0, rows), pl.ds(rows, rows)]


def gated(gate, up, ds):
    sig = sigmoid(gate)
    silu = gate * sig
    ds = ds.astype(BF).astype(F32)
    return (silu * up).astype(BF), (ds * up * (sig + silu * (1.0 - sig))).astype(BF), (ds * silu).astype(BF)


def top_kernel(x_ref, dy_ref, wg, wu, wd, gu0_ref, s0_ref, h1_ref, a0_ref, a1_ref, dgu1_ref, dwd_ref, wgu, wdn, s_ref, acc, sem, dsem):
    i = pl.program_id(0)
    blocks = wd.shape[1] // LANES
    load_all(
        [c for k in (0, 1) for c in gate_up_copies(wg.at[k], wu.at[k], wgu.at[k], sem.at[k], blocks)]
        + [pltpu.make_async_copy(wd.at[k], wdn.at[k], dsem.at[k]) for k in (0, 1)]
    )

    @pl.when(i == 0)
    def _():
        acc[...] = jnp.zeros_like(acc)

    rows = halves(x_ref)
    for r in rows:
        x = x_ref[r, :].astype(F32)
        a0_ref[r, :] = (x * rms_scale(x)).astype(BF)
    for k, c in chunks(blocks):
        at = pl.ds(2 * LANES * k, 2 * LANES * c)
        for r in rows:
            gu = dot(a0_ref[r, :], wgu[0, :, at], ROWS)
            gu0_ref[r, at] = gu
            for b in range(c):
                gate, up = (gu[:, (2 * b + j) * LANES : (2 * b + j + 1) * LANES] for j in (0, 1))
                s0_ref[r, pl.ds((k + b) * LANES, LANES)] = (gate * sigmoid(gate) * up).astype(BF)
    for r in rows:
        h = x_ref[r, :].astype(F32) + dot(s0_ref[r, :], wdn[0], ROWS).astype(BF).astype(F32)
        h = h.astype(BF)
        h1_ref[r, :] = h
        h = h.astype(F32)
        a1_ref[r, :] = (h * rms_scale(h)).astype(BF)
    for k, c in chunks(blocks):
        at = pl.ds(2 * LANES * k, 2 * LANES * c)
        for r in rows:
            gu = dot(a1_ref[r, :], wgu[1, :, at], ROWS)
            ds = dot(dy_ref[r, :], wdn[1, pl.ds(LANES * k, LANES * c), :], BY_T)
            for b in range(c):
                gate, up = (gu[:, (2 * b + j) * LANES : (2 * b + j + 1) * LANES] for j in (0, 1))
                s, dgate, dup = gated(gate, up, ds[:, b * LANES : (b + 1) * LANES])
                s_ref[r, pl.ds((k + b) * LANES, LANES)] = s
                dgu1_ref[r, pl.ds(2 * (k + b) * LANES, LANES)] = dgate
                dgu1_ref[r, pl.ds((2 * (k + b) + 1) * LANES, LANES)] = dup
    acc[...] += dot(s_ref[...], dy_ref[...], T_BY)

    @pl.when(i == pl.num_programs(0) - 1)
    def _():
        dwd_ref[...] = acc[...].astype(BF)


def back_of_chunk(dh_ref, a_ref, gu_ref, wd_ref, dgu_ref, acc, blocks, keep):
    i = pl.program_id(0)
    tokens = gu_ref.shape[0]
    part = tokens // 4

    def run(c, half):
        wide = pl.ds(0, 2 * c * LANES)

        def hidden(k):
            r, everywhere = pl.ds(k * part, part), pl.ds(half * tokens + k * part, part)
            ds = dot(dh_ref[everywhere, :], wd_ref[0, pl.ds(0, c * LANES), :], BY_T)
            for b in range(c):
                at = [pl.ds((2 * b + j) * LANES, LANES) for j in (0, 1)]
                _, dgate, dup = gated(gu_ref[r, at[0]], gu_ref[r, at[1]], ds[:, b * LANES : (b + 1) * LANES])
                dgu_ref[r, at[0]] = dgate
                dgu_ref[r, at[1]] = dup

        def weights(k):
            r, everywhere = pl.ds(k * part, part), pl.ds(half * tokens + k * part, part)
            term = dot(a_ref[everywhere, :], dgu_ref[r, wide], T_BY)
            if half == 0 and k == 0:
                acc[:, wide] = term
            else:
                acc[:, wide] += term

        for k in range(4):
            hidden(k)
            if k > 0:
                weights(k - 1)
        weights(3)
        if half == 1:
            keep(i // 2, 2 * c * LANES, acc[:, wide].astype(BF))

    whole_chunks = blocks // 2
    for half in (0, 1):

        @pl.when((i < 2 * whole_chunks) & (lax.rem(i, 2) == half))
        def _(half=half):
            run(2, half)

        if blocks % 2:

            @pl.when(i == 2 * whole_chunks + half)
            def _(half=half):
                run(1, half)


def gu_kernel(n, steps, todo, early, a_ref, dgu_ref, own_hbm, dw_ref, sum_ref, early_ref, own, load_sem, own_gu, *ring_refs):
    i = pl.program_id(0)
    width = dgu_ref.shape[1]
    rings = [Ring(n, own, *ring_refs[:3]), Ring(n, own_gu, *ring_refs[3:])]
    load = pltpu.make_async_copy(own_hbm, own, load_sem)

    @pl.when(i == 0)
    def _():
        load.start()
        greet(n, (1, -1))
        load.wait()
        rings[0].start()

    run_plan(todo, rings, steps)

    @pl.when(i == early)
    def _():
        rings[1].start()

    dw = dot(a_ref[...], dgu_ref[...], T_BY).astype(BF)
    dw_ref[...] = dw

    @pl.when(i < early)
    def _():
        own_gu[:, pl.ds(pl.multiple_of(i * width, width), width)] = dw_ref[...]

    @pl.when(i == steps - 1)
    def _():
        rest_of_plan(todo, rings, steps)
        rings[0].finish(sum_ref)
        rings[1].finish(early_ref)


def mid_kernel(
    n, steps, todo, h1_ref, dy_ref, dgu1_ref, s0_ref, wg, wu, own_hbm, dh_ref, dwd_ref, sum_ref, wgu, acc, sem, *ring,
):
    i = pl.program_id(0)
    own_cols = ring[0].shape[1]
    own_hbm = own_hbm.at[:, pl.ds(wgu.shape[1] - own_cols, own_cols)]
    close = with_ring(n, steps, todo, ring, own_hbm, sum_ref)
    load_all(gate_up_copies(wg.at[1], wu.at[1], wgu, sem, wg.shape[2] // LANES))

    @pl.when(i == 0)
    def _():
        acc[...] = jnp.zeros_like(acc)

    for r in halves(h1_ref):
        da = dot(dgu1_ref[r, :], wgu[...], BY_T).astype(BF).astype(F32)
        h = h1_ref[r, :].astype(F32)
        scale = rms_scale(h)
        back = scale * (da - h * (scale * scale * jnp.mean(da * h, -1, keepdims=True)))
        dh_ref[r, :] = (dy_ref[r, :].astype(F32) + back.astype(BF).astype(F32)).astype(BF)
    acc[...] += dot(s0_ref[...], dh_ref[...], T_BY)

    @pl.when(i == steps - 1)
    def _():
        dwd_ref[...] = acc[...].astype(BF)

    close()


def end_kernel(
    n, steps, todo, groups, count,
    dh_ref, a_ref, gu_ref, wd_ref, d0_hbm, gu1_early, gu1, d1, wg, wu, wd, mg, mu, md, vg, vu, vd,
    out_g, out_u, out_d, mb_g, mb_u, mb_d, vb_g, vb_u, vb_d,
    dgu_ref, acc, all_g, all_u, all_d, own_gu, own_d, gbuf, dbuf, wb_g, wb_d, sq_send, sq_all, in_sem, sq_s, sq_r, ag_s, ag_r, put_sem, *ring_refs,
):
    i = pl.program_id(0)
    me = lax.axis_index("dp")
    d = md.shape[2]
    rg, rd = mg.shape[1], md.shape[1]
    my_g = pl.ds(pl.multiple_of(me * rg, rg), rg)
    my_d = pl.ds(pl.multiple_of(me * rd, rd), rd)
    width = gu_ref.shape[1]
    early = gu1_early.shape[1]
    blocks = wg.shape[2] // LANES
    rings = [Ring(n, own_d, *ring_refs[:3])]
    for k, ((first, wide), _) in enumerate(groups):
        rings.append(Ring(n, own_gu.at[:, pl.ds(first * 2 * LANES, wide * 2 * LANES)], *ring_refs[3 * k + 3 : 3 * k + 6]))
    load = pltpu.make_async_copy(d0_hbm, own_d, in_sem.at[0])
    loads = [
        pltpu.make_async_copy(gu1_early, gbuf.at[1, :, pl.ds(0, early)], in_sem.at[12]),
        pltpu.make_async_copy(gu1, gbuf.at[1, :, pl.ds(early, gbuf.shape[2] - early)], in_sem.at[1]),
        pltpu.make_async_copy(d1, dbuf.at[1], in_sem.at[2]),
        pltpu.make_async_copy(mg, mb_g, in_sem.at[3]),
        pltpu.make_async_copy(mu, mb_u, in_sem.at[4]),
        pltpu.make_async_copy(md, mb_d, in_sem.at[5]),
        pltpu.make_async_copy(vg, vb_g, in_sem.at[6]),
        pltpu.make_async_copy(vu, vb_u, in_sem.at[7]),
        pltpu.make_async_copy(vd, vb_d, in_sem.at[8]),
        pltpu.make_async_copy(wg.at[:, my_g], wb_g.at[0], in_sem.at[9]),
        pltpu.make_async_copy(wu.at[:, my_g], wb_g.at[1], in_sem.at[10]),
        pltpu.make_async_copy(wd.at[:, my_d], wb_d, in_sem.at[11]),
    ]

    @pl.when(i == 0)
    def _():
        load.start()
        greet(n, tuple(range(1, n)))
        load.wait()
        rings[0].start()
        for c in loads:
            c.start()

    run_plan(todo, rings, steps)
    for k, (_, at) in enumerate(groups):
        if at < steps:

            @pl.when(i == at)
            def _(k=k):
                rings[k + 1].start()

    def keep(chunk, wide, dw):
        own_gu[:, pl.ds(pl.multiple_of(chunk * width, width), wide)] = dw

    back_of_chunk(dh_ref, a_ref, gu_ref, wd_ref, dgu_ref, acc, blocks, keep)

    @pl.when(i == steps - 1)
    def _():
        for c in loads:
            c.wait()
        for k, (_, at) in enumerate(groups):
            if at >= steps:
                rings[k + 1].start()
        rest_of_plan(todo, rings, steps)
        rings[0].finish(dbuf.at[0])
        for k, ((first, wide), _) in enumerate(groups):
            rings[k + 1].finish(gbuf.at[0, :, pl.ds(first * 2 * LANES, wide * 2 * LANES)])

        def squares(t):
            t = t.astype(F32)
            t = t * t
            t = jnp.sum(t.reshape(t.shape[0] // 8, 8, t.shape[1]), 0)
            return sum(t[:, k : k + LANES] for k in range(0, t.shape[1], LANES))

        sq = squares(gbuf[0]) + squares(gbuf[1]) + squares(dbuf[0]) + squares(dbuf[1])
        sq_send[...] = sq
        to_all = [
            pltpu.make_async_remote_copy(
                src_ref=sq_send,
                dst_ref=sq_all.at[k - 1],
                send_sem=sq_s.at[k - 1],
                recv_sem=sq_r.at[k - 1],
                device_id={"dp": lax.rem(me + k, n)},
                device_id_type=MESH,
            )
            for k in range(1, n)
        ]
        for c in to_all:
            c.start()
        for c in to_all:
            c.wait_recv()
        total = jnp.sum(sq + jnp.sum(sq_all[...], 0), keepdims=True)
        factor = jnp.minimum(1.0, 0.5 * lax.rsqrt(total / count + 1e-30))

        streams = rings[0].streams

        def gathered(layer, down, half, owner, to=(all_g, all_u, all_d)):
            owner = lax.rem(owner + n, n)
            if down:
                return to[2].at[layer, pl.ds(pl.multiple_of(owner * rd, rd), rd), pl.ds(half * (d // 2), d // 2)]
            return to[half].at[layer, pl.ds(pl.multiple_of(owner * rg, rg), rg)]

        def put(layer, down, s, hop):
            half, way, _ = streams[s]
            where = layer, down, half, me - way * hop
            sem = put_sem.at[layer * 2 + down, s, hop]
            return pltpu.make_async_copy(gathered(*where), gathered(*where, (out_g, out_u, out_d)), sem)

        def copy(layer, down, s, hop, owner):
            part = gathered(layer, down, streams[s][0], owner)
            return pltpu.make_async_remote_copy(
                src_ref=part,
                dst_ref=part,
                send_sem=ag_s.at[layer * 2 + down, s, hop - 1],
                recv_sem=ag_r.at[layer * 2 + down, s, hop - 1],
                device_id={"dp": lax.rem(me + streams[s][1] + n, n)},
                device_id_type=MESH,
            )

        def sending(layer, down, s, hop):
            return copy(layer, down, s, hop, me - streams[s][1] * (hop - 1))

        def arrival(layer, down, s, hop):
            return copy(layer, down, s, hop, me - streams[s][1] * hop)

        def adamw(w_ref, m_ref, v_ref, g, out):
            g = g.astype(F32) * factor
            m = 0.9 * m_ref[...] + 0.1 * g
            v = 0.95 * v_ref[...] + 0.05 * g * g
            w = w_ref[...].astype(F32)
            out[...] = (w - 0.02 * (m * lax.rsqrt(v + 1e-8) + 0.1 * w)).astype(BF)
            m_ref[...] = m
            v_ref[...] = v

        units = [(layer, down) for layer in (0, 1) for down in (0, 1)]
        for layer, down in units:
            if down:
                adamw(wb_d.at[layer], mb_d.at[layer], vb_d.at[layer], dbuf[layer], all_d.at[layer, my_d])
            else:
                for j, (m, v, to) in enumerate(((mb_g, vb_g, all_g), (mb_u, vb_u, all_u))):
                    g = [gbuf[layer, :, k : k + LANES] for k in range(j * LANES, gbuf.shape[2], 2 * LANES)]
                    adamw(wb_g.at[j, layer], m.at[layer], v.at[layer], jnp.concatenate(g, 1), to.at[layer, my_g])
            for s in range(4):
                sending(layer, down, s, 1).start()
            for s in (0, 1):
                put(layer, down, s, 0).start()
        for hop in range(1, streams[0][2] + 1):
            for layer, down in units:
                for s in range(4):
                    if hop <= streams[s][2]:
                        arrival(layer, down, s, hop).wait_recv()
                        if hop < streams[s][2]:
                            sending(layer, down, s, hop + 1).start()
                        put(layer, down, s, hop).start()
        for c in to_all:
            c.wait_send()
        for layer, down in units:
            for s in range(4):
                for hop in range(1, streams[s][2] + 1):
                    sending(layer, down, s, hop).wait_send()
                for hop in range(0 if s < 2 else 1, streams[s][2] + 1):
                    put(layer, down, s, hop).wait()


def store_kernel(*refs):
    k = len(refs) // 2
    copies = [pltpu.make_async_copy(a, b, refs[-1].at[j]) for j, (a, b) in enumerate(zip(refs[:k], refs[k : 2 * k]))]
    for c in copies:
        c.start()
    for c in copies:
        c.wait()


def params(cid=None, mib=62):
    if cid is None:
        return pltpu.CompilerParams(vmem_limit_bytes=mib << 20)
    return pltpu.CompilerParams(vmem_limit_bytes=mib << 20, collective_id=cid, has_side_effects=True)


def solution(mesh):
    n = mesh.shape["dp"]
    hops = n // 2, n - 1 - n // 2

    def step(x, dy, wg, wu, wd, mg, mu, md, vg, vu, vd):
        x, dy = x[0], dy[0]
        tokens, d = x.shape
        ff = wd.shape[1]
        rg, rd = d // n, ff // n
        tile = 512
        steps = tokens // tile
        blocks = ff // LANES
        rows = lambda c: pl.BlockSpec((tile, c), lambda i: (i, 0))
        whole = lambda *s: pl.BlockSpec(s, lambda i: (0,) * len(s))
        once = lambda *s: pl.BlockSpec(s, lambda i: (0,) * len(s), pipeline_mode=pl.Buffered(1))
        array = jax.ShapeDtypeStruct
        sem, vm = pltpu.SemaphoreType.DMA, pltpu.VMEM
        mm = 2 * tokens * d * ff

        def us(row_count, cols):
            return row_count * cols * 2 / 46.6e3

        def ring(row_count, cols):
            return [vm((4, hops[0], row_count, cols // 2), BF), sem((4, hops[0])), sem((4, hops[0]))]

        gu0, s0, h1, a0, a1, dgu1, dwd1 = pl.pallas_call(
            top_kernel,
            grid=(steps,),
            in_specs=[rows(d), rows(d), ANY, ANY, ANY],
            out_specs=[rows(2 * ff), rows(ff), rows(d), rows(d), rows(d), rows(2 * ff), whole(ff, d)],
            out_shape=[array((tokens, 2 * ff), F32), array((tokens, ff), BF)]
            + [array((tokens, d), BF)] * 3
            + [array((tokens, 2 * ff), BF), array((ff, d), BF)],
            scratch_shapes=[
                vm((2, d, 2 * ff), BF), vm((2, ff, d), BF), vm((tile, ff), BF), vm((ff, d), F32), sem((2, 2 * blocks)), sem((2,)),
            ],
            compiler_params=params(),
            cost_estimate=pl.CostEstimate(flops=7 * mm, bytes_accessed=100 << 20, transcendentals=0),
            name="top",
        )(x, dy, wg, wu, wd)

        pieces = 2 * -(-blocks // 2)
        of_chunk = lambda layer: [
            once(tokens, d),
            once(tokens, d),
            pl.BlockSpec((tokens // 2, 4 * LANES), lambda i: (lax.rem(i, 2), i // 2)),
            pl.BlockSpec((1, 2 * LANES, d), lambda i: (layer, i // 2, 0)),
        ]
        columns = lambda r: pl.BlockSpec((r, 2 * LANES), lambda i: (0, i))
        early = 3
        todo = plan(hops, [(0, us(rd, d // 2)), (early, us(rg, early * LANES))], blocks, 1.7)
        dwgu1, sum_d1, sum_early = pl.pallas_call(
            functools.partial(gu_kernel, n, blocks, todo, early),
            grid=(blocks,),
            in_specs=[once(tokens, d), columns(tokens), ANY],
            out_specs=[columns(d), whole(rd, d), whole(rg, 2 * LANES * early)],
            out_shape=[array((d, 2 * ff), BF), array((rd, d), BF), array((rg, 2 * LANES * early), BF)],
            scratch_shapes=[vm((ff, d), BF), sem(()), vm((d, 2 * LANES * early), BF)] + ring(rd, d) + ring(rg, 2 * LANES * early),
            compiler_params=params(0),
            cost_estimate=pl.CostEstimate(flops=2 * mm, bytes_accessed=30 << 20, transcendentals=0),
            name="gu1",
        )(a1, dgu1, dwd1)

        dh1, dwd0, sum_gu1 = pl.pallas_call(
            functools.partial(mid_kernel, n, steps, plan(hops, [(0, us(rg, ff - early * LANES))], steps, 3.5)),
            grid=(steps,),
            in_specs=[rows(d), rows(d), rows(2 * ff), rows(ff), ANY, ANY, ANY],
            out_specs=[rows(d), whole(ff, d), whole(rg, 2 * ff - 2 * LANES * early)],
            out_shape=[array((tokens, d), BF), array((ff, d), BF), array((rg, 2 * ff - 2 * LANES * early), BF)],
            scratch_shapes=[vm((d, 2 * ff), BF), vm((ff, d), F32), sem((2 * blocks,))]
            + [vm((d, 2 * ff - 2 * LANES * early), BF), sem(())]
            + ring(rg, 2 * ff - 2 * LANES * early),
            compiler_params=params(1),
            cost_estimate=pl.CostEstimate(flops=3 * mm, bytes_accessed=50 << 20, transcendentals=0),
            name="mid",
        )(h1, dy, dgu1, s0, wg, wu, dwgu1)

        groups = [(k, min(4, blocks - k)) for k in range(0, blocks, 4)]
        ready = [min(2 * -(-(f + w) // 2), pieces) for f, w in groups]
        todo = plan(hops, [(0, us(rd, d // 2))] + [(at, us(rg, w * LANES)) for at, (_, w) in zip(ready, groups)], pieces, 2.8)
        outs = pl.pallas_call(
            functools.partial(end_kernel, n, pieces, todo, list(zip(groups, ready)), float(wg.size + wu.size + wd.size)),
            grid=(pieces,),
            in_specs=of_chunk(0) + [ANY] * 13,
            out_specs=[pl.BlockSpec(memory_space=pltpu.VMEM)] * 9,
            out_shape=[vm(t.shape, BF) for t in (wg, wu, wd)] + [vm(t.shape, F32) for t in (mg, mu, md, vg, vu, vd)],
            scratch_shapes=[
                vm((tokens // 2, 4 * LANES), BF), vm((d, 4 * LANES), F32), vm(wg.shape, BF), vm(wu.shape, BF), vm(wd.shape, BF),
                vm((d, 2 * ff), BF), vm((ff, d), BF), vm((2, rg, 2 * ff), BF), vm((2, rd, d), BF),
                vm((2, *mg.shape), BF), vm(md.shape, BF), vm((8, LANES), F32), vm((n - 1, 8, LANES), F32),
                sem((13,)), sem((n - 1,)), sem((n - 1,)), sem((4, 4, hops[0])), sem((4, 4, hops[0])), sem((4, 4, hops[0] + 1)),
            ] + ring(rd, d) + [r for _, w in groups for r in ring(rg, w * 2 * LANES)],
            compiler_params=params(2, 48),
            cost_estimate=pl.CostEstimate(flops=2 * mm, bytes_accessed=30 << 20, transcendentals=0),
            name="end",
        )(dh1, a0, gu0, wd, dwd0, sum_early, sum_gu1, sum_d1, wg, wu, wd, mg, mu, md, vg, vu, vd)
        return tuple(
            pl.pallas_call(
                store_kernel,
                in_specs=[pl.BlockSpec(memory_space=pltpu.VMEM)] * 9,
                out_specs=[ANY] * 9,
                out_shape=[array(t.shape, t.dtype) for t in outs],
                scratch_shapes=[sem((9,))],
                compiler_params=params(None, 2),
                name="store",
            )(*outs)
        )

    seq, whole, rows = P(("rep", "dp"), None, None), P(None, None, None), P(None, "dp", None)
    return jax.shard_map(
        step,
        mesh=mesh,
        in_specs=(seq, seq) + (whole,) * 3 + (rows,) * 6,
        out_specs=(P("rep", None, None),) * 3 + (P("rep", "dp", None),) * 6,
        check_vma=False,
    )
```

```python
import functools

import jax
import jax.numpy as jnp
from jax import lax
from jax.experimental import pallas as pl
from jax.experimental.pallas import tpu as pltpu
from jax.sharding import PartitionSpec as P

BF, F32 = jnp.bfloat16, jnp.float32
MESH = pl.DeviceIdType.MESH
ANY = pl.BlockSpec(memory_space=pl.ANY)
ROWS = (((1,), (0,)), ((), ()))
BY_T = (((1,), (1,)), ((), ()))
T_BY = (((0,), (0,)), ((), ()))


def dot(a, b, dims):
    return lax.dot_general(a, b, dims, preferred_element_type=F32)


def rms_scale(wide):
    return lax.rsqrt(jnp.mean(wide * wide, -1, keepdims=True) + 1e-6)


def sigmoid(t):
    return 1.0 / (1.0 + jnp.exp(-t))


class Ring:
    def __init__(self, n, own, recv, send_sem, recv_sem):
        self.n, self.own, self.recv, self.send_sem, self.recv_sem = n, own, recv, send_sem, recv_sem
        self.rows, self.half = recv.shape[2], recv.shape[3]
        far, near = n // 2, n - 1 - n // 2
        self.streams = ((0, 1, far), (1, -1, far), (1, 1, near), (0, -1, near))
        self.me = lax.axis_index("dp")

    def mine(self, owner, half):
        owner = lax.rem(owner + self.n, self.n)
        rows = pl.ds(pl.multiple_of(owner * self.rows, self.rows), self.rows)
        return self.own.at[rows, pl.ds(half * self.half, self.half)]

    def copy(self, s, hop):
        half, way, hops = self.streams[s]
        src = self.mine(self.me + way * hops, half) if hop == 1 else self.recv.at[s, hop - 2]
        to = lax.rem(self.me + way + self.n, self.n)
        return pltpu.make_async_remote_copy(
            src_ref=src,
            dst_ref=self.recv.at[s, hop - 1],
            send_sem=self.send_sem.at[s, hop - 1],
            recv_sem=self.recv_sem.at[s, hop - 1],
            device_id={"dp": to},
            device_id_type=MESH,
        )

    def start(self):
        for s in range(4):
            self.copy(s, 1).start()

    def add(self, s, hop):
        half, way, hops = self.streams[s]
        self.copy(s, hop).wait_recv()
        if hop < hops:
            buf = self.recv.at[s, hop - 1]
            term = self.mine(self.me + way * (hops - hop), half)
            buf[...] = (buf[...].astype(F32) + term[...].astype(F32)).astype(BF)

    def send(self, s, hop):
        if hop < self.streams[s][2]:
            self.copy(s, hop + 1).start()

    def handle(self, pair):
        for s, hop in pair:
            self.add(s, hop)
        for s, hop in pair:
            self.send(s, hop)

    def finish(self, out):
        for half in (0, 1):
            total = self.mine(self.me, half)[...].astype(F32)
            for s, (its, _, hops) in enumerate(self.streams):
                if its == half:
                    total = total + self.recv[s, hops - 1].astype(F32)
            out[:, pl.ds(half * self.half, self.half)] = total.astype(BF)
        for s, (_, _, hops) in enumerate(self.streams):
            for hop in range(1, hops + 1):
                self.copy(s, hop).wait_send()


def greet(n, others):
    me = lax.axis_index("dp")
    barrier = pltpu.get_barrier_semaphore()
    for d in others:
        pl.semaphore_signal(barrier, inc=1, device_id={"dp": lax.rem(me + d + n, n)}, device_id_type=MESH)
    pl.semaphore_wait(barrier, len(others))


def plan(hops, rings, steps, step_us):
    latency, free, waiting, out = 2.5, 0.0, [], []
    far, near = hops

    def send(ring, group, hop, now):
        nonlocal free
        free = max(free, now) + rings[ring][1]
        waiting.append((free + latency, ring, group, hop))

    step, now = 0, 0.0
    while step < steps or waiting:
        if step < steps:
            now = step * step_us
        else:
            now = max(steps * step_us, min(w[0] for w in waiting))
        for w in sorted(w for w in waiting if w[0] <= now):
            waiting.remove(w)
            _, ring, group, hop = w
            out.append((min(step, steps), ring, tuple((s, hop) for s in ((0, 1), (2, 3))[group])))
            if hop < (far, near)[group]:
                send(ring, group, hop + 1, now)
        for ring, (start, _) in enumerate(rings):
            if start == step:
                send(ring, 0, 1, now)
                send(ring, 1, 1, now)
        step += 1
    return out


def run_plan(todo, rings, steps):
    i = pl.program_id(0)
    for step in range(1, steps):
        now = [(r, pair) for at, r, pair in todo if at == step]
        if now:

            @pl.when(i == step)
            def _(now=now):
                for r, pair in now:
                    rings[r].handle(pair)


def rest_of_plan(todo, rings, steps):
    for at, r, pair in todo:
        if at >= steps:
            rings[r].handle(pair)


def with_rings(n, steps, todo, own, load_sem, columns, refs, own_hbm, out):
    i = pl.program_id(0)
    rings = [Ring(n, own.at[:, pl.ds(*c)], *refs[3 * k : 3 * k + 3]) for k, c in enumerate(columns)]
    load = pltpu.make_async_copy(own_hbm, own, load_sem)

    @pl.when(i == 0)
    def _():
        load.start()
        greet(n, (1, -1))
        load.wait()
        for ring in rings:
            ring.start()

    run_plan(todo, rings, steps)

    def close():
        @pl.when(i == steps - 1)
        def _():
            rest_of_plan(todo, rings, steps)
            for ring, c in zip(rings, columns):
                ring.finish(out.at[:, pl.ds(*c)])

    return close


def load_all(copies):
    @pl.when(pl.program_id(0) == 0)
    def _():
        for c in copies:
            c.start()
        for c in copies:
            c.wait()


LANES = 128


def gate_up_copies(wg, wu, wgu, sem, blocks):
    out = []
    for k in range(blocks):
        for j, w in enumerate((wg, wu)):
            to = wgu.at[:, pl.ds(LANES * (2 * k + j), LANES)]
            out.append(pltpu.make_async_copy(w.at[:, pl.ds(LANES * k, LANES)], to, sem.at[2 * k + j]))
    return out


def chunks(blocks):
    return [(k, min(2, blocks - k)) for k in range(0, blocks, 2)]


def halves(ref):
    rows = ref.shape[0] // 2
    return [pl.ds(0, rows), pl.ds(rows, rows)]


def gated(gate, up, ds):
    sig = sigmoid(gate)
    silu = gate * sig
    ds = ds.astype(BF).astype(F32)
    return (silu * up).astype(BF), (ds * up * (sig + silu * (1.0 - sig))).astype(BF), (ds * silu).astype(BF)


def top_kernel(x_ref, dy_ref, wg, wu, wd, gu0_ref, s0_ref, h1_ref, a0_ref, a1_ref, dgu1_ref, dwd_ref, wgu, wdn, s_ref, acc, sem, dsem):
    i = pl.program_id(0)
    blocks = wd.shape[1] // LANES
    load_all(
        [c for k in (0, 1) for c in gate_up_copies(wg.at[k], wu.at[k], wgu.at[k], sem.at[k], blocks)]
        + [pltpu.make_async_copy(wd.at[k], wdn.at[k], dsem.at[k]) for k in (0, 1)]
    )

    @pl.when(i == 0)
    def _():
        acc[...] = jnp.zeros_like(acc)

    rows = halves(x_ref)
    for r in rows:
        x = x_ref[r, :].astype(F32)
        a0_ref[r, :] = (x * rms_scale(x)).astype(BF)
    for k, c in chunks(blocks):
        at = pl.ds(2 * LANES * k, 2 * LANES * c)
        for r in rows:
            gu = dot(a0_ref[r, :], wgu[0, :, at], ROWS)
            gu0_ref[r, at] = gu
            for b in range(c):
                gate, up = (gu[:, (2 * b + j) * LANES : (2 * b + j + 1) * LANES] for j in (0, 1))
                s0_ref[r, pl.ds((k + b) * LANES, LANES)] = (gate * sigmoid(gate) * up).astype(BF)
    for r in rows:
        h = x_ref[r, :].astype(F32) + dot(s0_ref[r, :], wdn[0], ROWS).astype(BF).astype(F32)
        h = h.astype(BF)
        h1_ref[r, :] = h
        h = h.astype(F32)
        a1_ref[r, :] = (h * rms_scale(h)).astype(BF)
    for k, c in chunks(blocks):
        at = pl.ds(2 * LANES * k, 2 * LANES * c)
        for r in rows:
            gu = dot(a1_ref[r, :], wgu[1, :, at], ROWS)
            ds = dot(dy_ref[r, :], wdn[1, pl.ds(LANES * k, LANES * c), :], BY_T)
            for b in range(c):
                gate, up = (gu[:, (2 * b + j) * LANES : (2 * b + j + 1) * LANES] for j in (0, 1))
                s, dgate, dup = gated(gate, up, ds[:, b * LANES : (b + 1) * LANES])
                s_ref[r, pl.ds((k + b) * LANES, LANES)] = s
                dgu1_ref[r, pl.ds(2 * (k + b) * LANES, LANES)] = dgate
                dgu1_ref[r, pl.ds((2 * (k + b) + 1) * LANES, LANES)] = dup
    acc[...] += dot(s_ref[...], dy_ref[...], T_BY)

    @pl.when(i == pl.num_programs(0) - 1)
    def _():
        dwd_ref[...] = acc[...].astype(BF)


def back_of_chunk(dh_ref, a_ref, gu_ref, wd_ref, dgu_ref, acc, blocks, keep):
    i = pl.program_id(0)
    tokens = gu_ref.shape[0]
    part = tokens // 4

    def run(c, half):
        wide = pl.ds(0, 2 * c * LANES)

        def hidden(k):
            r, everywhere = pl.ds(k * part, part), pl.ds(half * tokens + k * part, part)
            ds = dot(dh_ref[everywhere, :], wd_ref[0, pl.ds(0, c * LANES), :], BY_T)
            for b in range(c):
                at = [pl.ds((2 * b + j) * LANES, LANES) for j in (0, 1)]
                _, dgate, dup = gated(gu_ref[r, at[0]], gu_ref[r, at[1]], ds[:, b * LANES : (b + 1) * LANES])
                dgu_ref[r, at[0]] = dgate
                dgu_ref[r, at[1]] = dup

        def weights(k):
            r, everywhere = pl.ds(k * part, part), pl.ds(half * tokens + k * part, part)
            term = dot(a_ref[everywhere, :], dgu_ref[r, wide], T_BY)
            if half == 0 and k == 0:
                acc[:, wide] = term
            else:
                acc[:, wide] += term

        for k in range(4):
            hidden(k)
            if k > 0:
                weights(k - 1)
        weights(3)
        if half == 1:
            keep(i // 2, 2 * c * LANES, acc[:, wide].astype(BF))

    whole_chunks = blocks // 2
    for half in (0, 1):

        @pl.when((i < 2 * whole_chunks) & (lax.rem(i, 2) == half))
        def _(half=half):
            run(2, half)

        if blocks % 2:

            @pl.when(i == 2 * whole_chunks + half)
            def _(half=half):
                run(1, half)


def gu_kernel(n, steps, todo, a_ref, dgu_ref, own_hbm, dw_ref, sum_ref, own, load_sem, *ring):
    close = with_rings(n, steps, todo, own, load_sem, ((0, own.shape[1]),), ring, own_hbm, sum_ref)
    dw_ref[...] = dot(a_ref[...], dgu_ref[...], T_BY).astype(BF)
    close()


def mid_kernel(
    n, steps, todo, columns, h1_ref, dy_ref, dgu1_ref, s0_ref, wg, wu, own_hbm, dh_ref, dwd_ref, sum_ref,
    wgu, acc, sem, own, load_sem, *ring,
):
    i = pl.program_id(0)
    close = with_rings(n, steps, todo, own, load_sem, columns, ring, own_hbm, sum_ref)
    load_all(gate_up_copies(wg.at[1], wu.at[1], wgu, sem, wg.shape[2] // LANES))

    @pl.when(i == 0)
    def _():
        acc[...] = jnp.zeros_like(acc)

    for r in halves(h1_ref):
        da = dot(dgu1_ref[r, :], wgu[...], BY_T).astype(BF).astype(F32)
        h = h1_ref[r, :].astype(F32)
        scale = rms_scale(h)
        back = scale * (da - h * (scale * scale * jnp.mean(da * h, -1, keepdims=True)))
        dh_ref[r, :] = (dy_ref[r, :].astype(F32) + back.astype(BF).astype(F32)).astype(BF)
    acc[...] += dot(s0_ref[...], dh_ref[...], T_BY)

    @pl.when(i == steps - 1)
    def _():
        dwd_ref[...] = acc[...].astype(BF)

    close()


def end_kernel(
    n, steps, todo, groups, count,
    dh_ref, a_ref, gu_ref, wd_ref, d0_hbm, gu1, d1, wg, wu, wd, mg, mu, md, vg, vu, vd,
    out_g, out_u, out_d, mb_g, mb_u, mb_d, vb_g, vb_u, vb_d,
    dgu_ref, acc, all_g, all_u, all_d, own_gu, own_d, gbuf, dbuf, wb_g, wb_d, sq_send, sq_all, in_sem, sq_s, sq_r, ag_s, ag_r, put_sem, direct, direct_s, direct_r, *ring_refs,
):
    i = pl.program_id(0)
    me = lax.axis_index("dp")
    d = md.shape[2]
    rg, rd = mg.shape[1], md.shape[1]
    my_g = pl.ds(pl.multiple_of(me * rg, rg), rg)
    my_d = pl.ds(pl.multiple_of(me * rd, rd), rd)
    width = gu_ref.shape[1]
    blocks = wg.shape[2] // LANES
    last = pl.ds(2 * LANES * (blocks - 1), 2 * LANES)
    rings = [Ring(n, own_d, *ring_refs[:3])]
    for k, ((first, wide), _) in enumerate(groups):
        rings.append(Ring(n, own_gu.at[:, pl.ds(first * 2 * LANES, wide * 2 * LANES)], *ring_refs[3 * k + 3 : 3 * k + 6]))
    load = pltpu.make_async_copy(d0_hbm, own_d, in_sem.at[0])
    loads = [
        pltpu.make_async_copy(gu1, gbuf.at[1], in_sem.at[1]),
        pltpu.make_async_copy(d1, dbuf.at[1], in_sem.at[2]),
        pltpu.make_async_copy(mg, mb_g, in_sem.at[3]),
        pltpu.make_async_copy(mu, mb_u, in_sem.at[4]),
        pltpu.make_async_copy(md, mb_d, in_sem.at[5]),
        pltpu.make_async_copy(vg, vb_g, in_sem.at[6]),
        pltpu.make_async_copy(vu, vb_u, in_sem.at[7]),
        pltpu.make_async_copy(vd, vb_d, in_sem.at[8]),
        pltpu.make_async_copy(wg.at[:, my_g], wb_g.at[0], in_sem.at[9]),
        pltpu.make_async_copy(wu.at[:, my_g], wb_g.at[1], in_sem.at[10]),
        pltpu.make_async_copy(wd.at[:, my_d], wb_d, in_sem.at[11]),
    ]

    @pl.when(i == 0)
    def _():
        load.start()
        greet(n, tuple(range(1, n)))
        load.wait()
        rings[0].start()
        for c in loads:
            c.start()

    run_plan(todo, rings, steps)
    for k, (_, at) in enumerate(groups):
        if at < steps:

            @pl.when(i == at)
            def _(k=k):
                rings[k + 1].start()

    def keep(chunk, wide, dw):
        own_gu[:, pl.ds(pl.multiple_of(chunk * width, width), wide)] = dw

    back_of_chunk(dh_ref, a_ref, gu_ref, wd_ref, dgu_ref, acc, blocks, keep)

    @pl.when(i == steps - 1)
    def _():
        straight = []
        for k in range(1, n):
            to = lax.rem(me + k, n)
            straight.append(
                pltpu.make_async_remote_copy(
                    src_ref=own_gu.at[pl.ds(pl.multiple_of(to * rg, rg), rg), last],
                    dst_ref=direct.at[k - 1],
                    send_sem=direct_s.at[k - 1],
                    recv_sem=direct_r.at[k - 1],
                    device_id={"dp": to},
                    device_id_type=MESH,
                )
            )
        for c in loads:
            c.wait()
        for c in straight:
            c.start()
        rest_of_plan(todo, rings, steps)
        for c in straight:
            c.wait_recv()
        own_terms = own_gu[my_g, last].astype(F32)
        gbuf[0, :, last] = (own_terms + jnp.sum(direct[...].astype(F32), 0)).astype(BF)
        rings[0].finish(dbuf.at[0])
        for k, ((first, wide), _) in enumerate(groups):
            rings[k + 1].finish(gbuf.at[0, :, pl.ds(first * 2 * LANES, wide * 2 * LANES)])

        def squares(t):
            t = t.astype(F32)
            t = t * t
            t = jnp.sum(t.reshape(t.shape[0] // 8, 8, t.shape[1]), 0)
            return sum(t[:, k : k + LANES] for k in range(0, t.shape[1], LANES))

        sq = squares(gbuf[0]) + squares(gbuf[1]) + squares(dbuf[0]) + squares(dbuf[1])
        sq_send[...] = sq
        to_all = [
            pltpu.make_async_remote_copy(
                src_ref=sq_send,
                dst_ref=sq_all.at[k - 1],
                send_sem=sq_s.at[k - 1],
                recv_sem=sq_r.at[k - 1],
                device_id={"dp": lax.rem(me + k, n)},
                device_id_type=MESH,
            )
            for k in range(1, n)
        ]
        for c in to_all:
            c.start()
        for c in to_all:
            c.wait_recv()
        total = jnp.sum(sq + jnp.sum(sq_all[...], 0), keepdims=True)
        factor = jnp.minimum(1.0, 0.5 * lax.rsqrt(total / count + 1e-30))

        streams = rings[0].streams

        def gathered(layer, down, half, owner, to=(all_g, all_u, all_d)):
            owner = lax.rem(owner + n, n)
            if down:
                return to[2].at[layer, pl.ds(pl.multiple_of(owner * rd, rd), rd), pl.ds(half * (d // 2), d // 2)]
            return to[half].at[layer, pl.ds(pl.multiple_of(owner * rg, rg), rg)]

        def put(layer, down, s, hop):
            half, way, _ = streams[s]
            where = layer, down, half, me - way * hop
            sem = put_sem.at[layer * 2 + down, s, hop]
            return pltpu.make_async_copy(gathered(*where), gathered(*where, (out_g, out_u, out_d)), sem)

        def copy(layer, down, s, hop, owner):
            part = gathered(layer, down, streams[s][0], owner)
            return pltpu.make_async_remote_copy(
                src_ref=part,
                dst_ref=part,
                send_sem=ag_s.at[layer * 2 + down, s, hop - 1],
                recv_sem=ag_r.at[layer * 2 + down, s, hop - 1],
                device_id={"dp": lax.rem(me + streams[s][1] + n, n)},
                device_id_type=MESH,
            )

        def sending(layer, down, s, hop):
            return copy(layer, down, s, hop, me - streams[s][1] * (hop - 1))

        def arrival(layer, down, s, hop):
            return copy(layer, down, s, hop, me - streams[s][1] * hop)

        def adamw(w_ref, m_ref, v_ref, g, out):
            g = g.astype(F32) * factor
            m = 0.9 * m_ref[...] + 0.1 * g
            v = 0.95 * v_ref[...] + 0.05 * g * g
            w = w_ref[...].astype(F32)
            out[...] = (w - 0.02 * (m * lax.rsqrt(v + 1e-8) + 0.1 * w)).astype(BF)
            m_ref[...] = m
            v_ref[...] = v

        units = [(layer, down) for layer in (0, 1) for down in (0, 1)]
        for layer, down in units:
            if down:
                adamw(wb_d.at[layer], mb_d.at[layer], vb_d.at[layer], dbuf[layer], all_d.at[layer, my_d])
            else:
                for j, (m, v, to) in enumerate(((mb_g, vb_g, all_g), (mb_u, vb_u, all_u))):
                    g = [gbuf[layer, :, k : k + LANES] for k in range(j * LANES, gbuf.shape[2], 2 * LANES)]
                    adamw(wb_g.at[j, layer], m.at[layer], v.at[layer], jnp.concatenate(g, 1), to.at[layer, my_g])
            for s in range(4):
                sending(layer, down, s, 1).start()
            for s in (0, 1):
                put(layer, down, s, 0).start()
        for hop in range(1, streams[0][2] + 1):
            for layer, down in units:
                for s in range(4):
                    if hop <= streams[s][2]:
                        arrival(layer, down, s, hop).wait_recv()
                        if hop < streams[s][2]:
                            sending(layer, down, s, hop + 1).start()
                        put(layer, down, s, hop).start()
        for c in to_all + straight:
            c.wait_send()
        for layer, down in units:
            for s in range(4):
                for hop in range(1, streams[s][2] + 1):
                    sending(layer, down, s, hop).wait_send()
                for hop in range(0 if s < 2 else 1, streams[s][2] + 1):
                    put(layer, down, s, hop).wait()


def store_kernel(*refs):
    k = len(refs) // 2
    copies = [pltpu.make_async_copy(a, b, refs[-1].at[j]) for j, (a, b) in enumerate(zip(refs[:k], refs[k : 2 * k]))]
    for c in copies:
        c.start()
    for c in copies:
        c.wait()


def params(cid=None, mib=62):
    if cid is None:
        return pltpu.CompilerParams(vmem_limit_bytes=mib << 20)
    return pltpu.CompilerParams(vmem_limit_bytes=mib << 20, collective_id=cid, has_side_effects=True)


def solution(mesh):
    n = mesh.shape["dp"]
    hops = n // 2, n - 1 - n // 2

    def step(x, dy, wg, wu, wd, mg, mu, md, vg, vu, vd):
        x, dy = x[0], dy[0]
        tokens, d = x.shape
        ff = wd.shape[1]
        rg, rd = d // n, ff // n
        tile = 512
        steps = tokens // tile
        blocks = ff // LANES
        rows = lambda c: pl.BlockSpec((tile, c), lambda i: (i, 0))
        whole = lambda *s: pl.BlockSpec(s, lambda i: (0,) * len(s))
        once = lambda *s: pl.BlockSpec(s, lambda i: (0,) * len(s), pipeline_mode=pl.Buffered(1))
        array = jax.ShapeDtypeStruct
        sem, vm = pltpu.SemaphoreType.DMA, pltpu.VMEM
        mm = 2 * tokens * d * ff

        def us(row_count, cols):
            return row_count * cols * 2 / 46.6e3

        def ring(row_count, cols):
            return [vm((4, hops[0], row_count, cols // 2), BF), sem((4, hops[0])), sem((4, hops[0]))]

        gu0, s0, h1, a0, a1, dgu1, dwd1 = pl.pallas_call(
            top_kernel,
            grid=(steps,),
            in_specs=[rows(d), rows(d), ANY, ANY, ANY],
            out_specs=[rows(2 * ff), rows(ff), rows(d), rows(d), rows(d), rows(2 * ff), whole(ff, d)],
            out_shape=[array((tokens, 2 * ff), F32), array((tokens, ff), BF)]
            + [array((tokens, d), BF)] * 3
            + [array((tokens, 2 * ff), BF), array((ff, d), BF)],
            scratch_shapes=[
                vm((2, d, 2 * ff), BF), vm((2, ff, d), BF), vm((tile, ff), BF), vm((ff, d), F32), sem((2, 2 * blocks)), sem((2,)),
            ],
            compiler_params=params(),
            cost_estimate=pl.CostEstimate(flops=7 * mm, bytes_accessed=100 << 20, transcendentals=0),
            name="top",
        )(x, dy, wg, wu, wd)

        pieces = 2 * -(-blocks // 2)
        of_chunk = lambda layer: [
            once(tokens, d),
            once(tokens, d),
            pl.BlockSpec((tokens // 2, 4 * LANES), lambda i: (lax.rem(i, 2), i // 2)),
            pl.BlockSpec((1, 2 * LANES, d), lambda i: (layer, i // 2, 0)),
        ]
        columns = lambda r: pl.BlockSpec((r, 2 * LANES), lambda i: (0, i))
        dwgu1, sum_d1 = pl.pallas_call(
            functools.partial(gu_kernel, n, blocks, plan(hops, [(0, us(rd, d // 2))], blocks, 1.8)),
            grid=(blocks,),
            in_specs=[once(tokens, d), columns(tokens), ANY],
            out_specs=[columns(d), whole(rd, d)],
            out_shape=[array((d, 2 * ff), BF), array((rd, d), BF)],
            scratch_shapes=[vm((ff, d), BF), sem(())] + ring(rd, d),
            compiler_params=params(0),
            cost_estimate=pl.CostEstimate(flops=2 * mm, bytes_accessed=30 << 20, transcendentals=0),
            name="gu1",
        )(a1, dgu1, dwd1)

        cut = blocks // 2 * 2 * LANES
        parts = ((0, cut), (cut, 2 * ff - cut))
        todo = plan(hops, [(0, us(rg, w // 2)) for _, w in parts], steps, 3.6)
        dh1, dwd0, sum_gu1 = pl.pallas_call(
            functools.partial(mid_kernel, n, steps, todo, parts),
            grid=(steps,),
            in_specs=[rows(d), rows(d), rows(2 * ff), rows(ff), ANY, ANY, ANY],
            out_specs=[rows(d), whole(ff, d), whole(rg, 2 * ff)],
            out_shape=[array((tokens, d), BF), array((ff, d), BF), array((rg, 2 * ff), BF)],
            scratch_shapes=[vm((d, 2 * ff), BF), vm((ff, d), F32), sem((2 * blocks,))]
            + [vm((d, 2 * ff), BF), sem(())]
            + [r for _, w in parts for r in ring(rg, w)],
            compiler_params=params(1),
            cost_estimate=pl.CostEstimate(flops=3 * mm, bytes_accessed=50 << 20, transcendentals=0),
            name="mid",
        )(h1, dy, dgu1, s0, wg, wu, dwgu1)

        groups = [(k, min(4, blocks - 1 - k)) for k in range(0, blocks - 1, 4)]
        ready = [min(2 * -(-(f + w) // 2), pieces) for f, w in groups]
        todo = plan(hops, [(0, us(rd, d // 2))] + [(at, us(rg, w * LANES)) for at, (_, w) in zip(ready, groups)], pieces, 2.8)
        outs = pl.pallas_call(
            functools.partial(end_kernel, n, pieces, todo, list(zip(groups, ready)), float(wg.size + wu.size + wd.size)),
            grid=(pieces,),
            in_specs=of_chunk(0) + [ANY] * 12,
            out_specs=[pl.BlockSpec(memory_space=pltpu.VMEM)] * 9,
            out_shape=[vm(t.shape, BF) for t in (wg, wu, wd)] + [vm(t.shape, F32) for t in (mg, mu, md, vg, vu, vd)],
            scratch_shapes=[
                vm((tokens // 2, 4 * LANES), BF), vm((d, 4 * LANES), F32), vm(wg.shape, BF), vm(wu.shape, BF), vm(wd.shape, BF),
                vm((d, 2 * ff), BF), vm((ff, d), BF), vm((2, rg, 2 * ff), BF), vm((2, rd, d), BF),
                vm((2, *mg.shape), BF), vm(md.shape, BF), vm((8, LANES), F32), vm((n - 1, 8, LANES), F32),
                sem((12,)), sem((n - 1,)), sem((n - 1,)), sem((4, 4, hops[0])), sem((4, 4, hops[0])), sem((4, 4, hops[0] + 1)),
                vm((n - 1, rg, 2 * LANES), BF), sem((n - 1,)), sem((n - 1,)),
            ] + ring(rd, d) + [r for _, w in groups for r in ring(rg, w * 2 * LANES)],
            compiler_params=params(2, 48),
            cost_estimate=pl.CostEstimate(flops=2 * mm, bytes_accessed=30 << 20, transcendentals=0),
            name="end",
        )(dh1, a0, gu0, wd, dwd0, sum_gu1, sum_d1, wg, wu, wd, mg, mu, md, vg, vu, vd)
        return tuple(
            pl.pallas_call(
                store_kernel,
                in_specs=[pl.BlockSpec(memory_space=pltpu.VMEM)] * 9,
                out_specs=[ANY] * 9,
                out_shape=[array(t.shape, t.dtype) for t in outs],
                scratch_shapes=[sem((9,))],
                compiler_params=params(None, 2),
                name="store",
            )(*outs)
        )

    seq, whole, rows = P(("rep", "dp"), None, None), P(None, None, None), P(None, "dp", None)
    return jax.shard_map(
        step,
        mesh=mesh,
        in_specs=(seq, seq) + (whole,) * 3 + (rows,) * 6,
        out_specs=(P("rep", None, None),) * 3 + (P("rep", "dp", None),) * 6,
        check_vma=False,
    )
```

```python
import functools

import jax
import jax.numpy as jnp
from jax import lax
from jax.experimental import pallas as pl
from jax.experimental.pallas import tpu as pltpu
from jax.sharding import PartitionSpec as P

BF, F32 = jnp.bfloat16, jnp.float32
MESH = pl.DeviceIdType.MESH
ANY = pl.BlockSpec(memory_space=pl.ANY)
ROWS = (((1,), (0,)), ((), ()))
BY_T = (((1,), (1,)), ((), ()))
T_BY = (((0,), (0,)), ((), ()))


def dot(a, b, dims):
    return lax.dot_general(a, b, dims, preferred_element_type=F32)


def rms_scale(wide):
    return lax.rsqrt(jnp.mean(wide * wide, -1, keepdims=True) + 1e-6)


def sigmoid(t):
    return 1.0 / (1.0 + jnp.exp(-t))


class Ring:
    def __init__(self, n, own, recv, send_sem, recv_sem):
        self.n, self.own, self.recv, self.send_sem, self.recv_sem = n, own, recv, send_sem, recv_sem
        self.rows, self.half = recv.shape[2], recv.shape[3]
        far, near = n // 2, n - 1 - n // 2
        self.streams = ((0, 1, far), (1, -1, far), (1, 1, near), (0, -1, near))
        self.me = lax.axis_index("dp")

    def mine(self, owner, half):
        owner = lax.rem(owner + self.n, self.n)
        rows = pl.ds(pl.multiple_of(owner * self.rows, self.rows), self.rows)
        return self.own.at[rows, pl.ds(half * self.half, self.half)]

    def copy(self, s, hop):
        half, way, hops = self.streams[s]
        src = self.mine(self.me + way * hops, half) if hop == 1 else self.recv.at[s, hop - 2]
        to = lax.rem(self.me + way + self.n, self.n)
        return pltpu.make_async_remote_copy(
            src_ref=src,
            dst_ref=self.recv.at[s, hop - 1],
            send_sem=self.send_sem.at[s, hop - 1],
            recv_sem=self.recv_sem.at[s, hop - 1],
            device_id={"dp": to},
            device_id_type=MESH,
        )

    def start(self):
        for s in range(4):
            self.copy(s, 1).start()

    def add(self, s, hop):
        half, way, hops = self.streams[s]
        self.copy(s, hop).wait_recv()
        if hop < hops:
            buf = self.recv.at[s, hop - 1]
            term = self.mine(self.me + way * (hops - hop), half)
            buf[...] = (buf[...].astype(F32) + term[...].astype(F32)).astype(BF)

    def send(self, s, hop):
        if hop < self.streams[s][2]:
            self.copy(s, hop + 1).start()

    def handle(self, pair):
        for s, hop in pair:
            self.add(s, hop)
        for s, hop in pair:
            self.send(s, hop)

    def finish(self, out):
        for half in (0, 1):
            total = self.mine(self.me, half)[...].astype(F32)
            for s, (its, _, hops) in enumerate(self.streams):
                if its == half:
                    total = total + self.recv[s, hops - 1].astype(F32)
            out[:, pl.ds(half * self.half, self.half)] = total.astype(BF)
        for s, (_, _, hops) in enumerate(self.streams):
            for hop in range(1, hops + 1):
                self.copy(s, hop).wait_send()


def greet(n, others):
    me = lax.axis_index("dp")
    barrier = pltpu.get_barrier_semaphore()
    for d in others:
        pl.semaphore_signal(barrier, inc=1, device_id={"dp": lax.rem(me + d + n, n)}, device_id_type=MESH)
    pl.semaphore_wait(barrier, len(others))


def plan(hops, rings, steps, step_us):
    latency, free, waiting, out = 3.0, 0.0, [], []
    far, near = hops

    def send(ring, group, hop, now):
        nonlocal free
        free = max(free, now) + rings[ring][1]
        waiting.append((free + latency, ring, group, hop))

    step, now = 0, 0.0
    while step < steps or waiting:
        if step < steps:
            now = step * step_us
        else:
            now = max(steps * step_us, min(w[0] for w in waiting))
        for w in sorted(w for w in waiting if w[0] <= now):
            waiting.remove(w)
            _, ring, group, hop = w
            out.append((min(step, steps), ring, tuple((s, hop) for s in ((0, 1), (2, 3))[group])))
            if hop < (far, near)[group]:
                send(ring, group, hop + 1, now)
        for ring, (start, _) in enumerate(rings):
            if start == step:
                send(ring, 0, 1, now)
                send(ring, 1, 1, now)
        step += 1
    return out


def ticks(todo, rings, steps, per_step, k, only=lambda step: True):
    i = pl.program_id(0)
    for step in range(steps):
        now = [(r, pair) for at, r, pair in todo if at == step * per_step + k]
        if now and only(step):

            @pl.when(i == step)
            def _(now=now):
                for r, pair in now:
                    rings[r].handle(pair)


def rest_of_plan(todo, rings, steps):
    for at, r, pair in todo:
        if at >= steps:
            rings[r].handle(pair)


def with_rings(n, steps, per_step, todo, own, load_sem, columns, refs, own_hbm, out):
    i = pl.program_id(0)
    rings = [Ring(n, own.at[:, pl.ds(*c)], *refs[3 * k : 3 * k + 3]) for k, c in enumerate(columns)]
    load = pltpu.make_async_copy(own_hbm, own, load_sem)

    @pl.when(i == 0)
    def _():
        load.start()
        greet(n, (1, -1))
        load.wait()
        for ring in rings:
            ring.start()

    ticks(todo, rings, steps, per_step, 0)

    def close():
        @pl.when(i == steps - 1)
        def _():
            rest_of_plan(todo, rings, steps * per_step)
            for ring, c in zip(rings, columns):
                ring.finish(out.at[:, pl.ds(*c)])

    return lambda k: ticks(todo, rings, steps, per_step, k), close


def load_all(copies):
    @pl.when(pl.program_id(0) == 0)
    def _():
        for c in copies:
            c.start()
        for c in copies:
            c.wait()


LANES = 128


def gate_up_copies(wg, wu, wgu, sem, blocks):
    out = []
    for k in range(blocks):
        for j, w in enumerate((wg, wu)):
            to = wgu.at[:, pl.ds(LANES * (2 * k + j), LANES)]
            out.append(pltpu.make_async_copy(w.at[:, pl.ds(LANES * k, LANES)], to, sem.at[2 * k + j]))
    return out


def chunks(blocks):
    return [(k, min(2, blocks - k)) for k in range(0, blocks, 2)]


def halves(ref):
    rows = ref.shape[0] // 2
    return [pl.ds(0, rows), pl.ds(rows, rows)]


def gated(gate, up, ds):
    sig = sigmoid(gate)
    silu = gate * sig
    ds = ds.astype(BF).astype(F32)
    return (silu * up).astype(BF), (ds * up * (sig + silu * (1.0 - sig))).astype(BF), (ds * silu).astype(BF)


def top_kernel(x_ref, dy_ref, wg, wu, wd, gu0_ref, s0_ref, h1_ref, a0_ref, a1_ref, dgu1_ref, dwd_ref, wgu, wdn, s_ref, acc, sem, dsem):
    i = pl.program_id(0)
    blocks = wd.shape[1] // LANES
    load_all(
        [c for k in (0, 1) for c in gate_up_copies(wg.at[k], wu.at[k], wgu.at[k], sem.at[k], blocks)]
        + [pltpu.make_async_copy(wd.at[k], wdn.at[k], dsem.at[k]) for k in (0, 1)]
    )

    @pl.when(i == 0)
    def _():
        acc[...] = jnp.zeros_like(acc)

    rows = halves(x_ref)
    for r in rows:
        x = x_ref[r, :].astype(F32)
        a0_ref[r, :] = (x * rms_scale(x)).astype(BF)
    for k, c in chunks(blocks):
        at = pl.ds(2 * LANES * k, 2 * LANES * c)
        for r in rows:
            gu = dot(a0_ref[r, :], wgu[0, :, at], ROWS)
            gu0_ref[r, at] = gu
            for b in range(c):
                gate, up = (gu[:, (2 * b + j) * LANES : (2 * b + j + 1) * LANES] for j in (0, 1))
                s0_ref[r, pl.ds((k + b) * LANES, LANES)] = (gate * sigmoid(gate) * up).astype(BF)
    for r in rows:
        h = x_ref[r, :].astype(F32) + dot(s0_ref[r, :], wdn[0], ROWS).astype(BF).astype(F32)
        h = h.astype(BF)
        h1_ref[r, :] = h
        h = h.astype(F32)
        a1_ref[r, :] = (h * rms_scale(h)).astype(BF)
    for k, c in chunks(blocks):
        at = pl.ds(2 * LANES * k, 2 * LANES * c)
        for r in rows:
            gu = dot(a1_ref[r, :], wgu[1, :, at], ROWS)
            ds = dot(dy_ref[r, :], wdn[1, pl.ds(LANES * k, LANES * c), :], BY_T)
            for b in range(c):
                gate, up = (gu[:, (2 * b + j) * LANES : (2 * b + j + 1) * LANES] for j in (0, 1))
                s, dgate, dup = gated(gate, up, ds[:, b * LANES : (b + 1) * LANES])
                s_ref[r, pl.ds((k + b) * LANES, LANES)] = s
                dgu1_ref[r, pl.ds(2 * (k + b) * LANES, LANES)] = dgate
                dgu1_ref[r, pl.ds((2 * (k + b) + 1) * LANES, LANES)] = dup
    acc[...] += dot(s_ref[...], dy_ref[...], T_BY)

    @pl.when(i == pl.num_programs(0) - 1)
    def _():
        dwd_ref[...] = acc[...].astype(BF)


def back_of_chunk(dh_ref, a_ref, gu_ref, wd_ref, dgu_ref, acc, blocks, keep, tick):
    i = pl.program_id(0)
    tokens = gu_ref.shape[0]
    part = tokens // 4
    whole_chunks = blocks // 2

    def run(c, half):
        wide = pl.ds(0, 2 * c * LANES)

        def hidden(k):
            r, everywhere = pl.ds(k * part, part), pl.ds(half * tokens + k * part, part)
            ds = dot(dh_ref[everywhere, :], wd_ref[0, pl.ds(0, c * LANES), :], BY_T)
            for b in range(c):
                at = [pl.ds((2 * b + j) * LANES, LANES) for j in (0, 1)]
                _, dgate, dup = gated(gu_ref[r, at[0]], gu_ref[r, at[1]], ds[:, b * LANES : (b + 1) * LANES])
                dgu_ref[r, at[0]] = dgate
                dgu_ref[r, at[1]] = dup

        def weights(k):
            r, everywhere = pl.ds(k * part, part), pl.ds(half * tokens + k * part, part)
            term = dot(a_ref[everywhere, :], dgu_ref[r, wide], T_BY)
            if half == 0 and k == 0:
                acc[:, wide] = term
            else:
                acc[:, wide] += term

        for k in range(4):
            if k > 0:
                tick(k, lambda step: step % 2 == half and (step < 2 * whole_chunks) == (c == 2))
            hidden(k)
            if k > 0:
                weights(k - 1)
        weights(3)
        if half == 1:
            keep(i // 2, 2 * c * LANES, acc[:, wide].astype(BF))

    for half in (0, 1):

        @pl.when((i < 2 * whole_chunks) & (lax.rem(i, 2) == half))
        def _(half=half):
            run(2, half)

        if blocks % 2:

            @pl.when(i == 2 * whole_chunks + half)
            def _(half=half):
                run(1, half)


def gu_kernel(n, steps, todo, a_ref, dgu_ref, own_hbm, dw_ref, sum_ref, own, load_sem, *ring):
    _, close = with_rings(n, steps, 1, todo, own, load_sem, ((0, own.shape[1]),), ring, own_hbm, sum_ref)
    dw_ref[...] = dot(a_ref[...], dgu_ref[...], T_BY).astype(BF)
    close()


def mid_kernel(
    n, steps, todo, columns, h1_ref, dy_ref, dgu1_ref, s0_ref, wg, wu, own_hbm, dh_ref, dwd_ref, sum_ref,
    wgu, acc, sem, own, load_sem, *ring,
):
    i = pl.program_id(0)
    tick, close = with_rings(n, steps, 2, todo, own, load_sem, columns, ring, own_hbm, sum_ref)
    load_all(gate_up_copies(wg.at[1], wu.at[1], wgu, sem, wg.shape[2] // LANES))

    @pl.when(i == 0)
    def _():
        acc[...] = jnp.zeros_like(acc)

    for r in halves(h1_ref):
        da = dot(dgu1_ref[r, :], wgu[...], BY_T).astype(BF).astype(F32)
        h = h1_ref[r, :].astype(F32)
        scale = rms_scale(h)
        back = scale * (da - h * (scale * scale * jnp.mean(da * h, -1, keepdims=True)))
        dh_ref[r, :] = (dy_ref[r, :].astype(F32) + back.astype(BF).astype(F32)).astype(BF)
    tick(1)
    acc[...] += dot(s0_ref[...], dh_ref[...], T_BY)

    @pl.when(i == steps - 1)
    def _():
        dwd_ref[...] = acc[...].astype(BF)

    close()


def end_kernel(
    n, steps, todo, groups, count,
    dh_ref, a_ref, gu_ref, wd_ref, d0_hbm, gu1, d1, wg, wu, wd, mg, mu, md, vg, vu, vd,
    out_g, out_u, out_d, mb_g, mb_u, mb_d, vb_g, vb_u, vb_d,
    dgu_ref, acc, all_g, all_u, all_d, own_gu, own_d, gbuf, dbuf, wb_g, wb_d, sq_send, sq_all, in_sem, sq_s, sq_r, ag_s, ag_r, put_sem, direct, direct_s, direct_r, *ring_refs,
):
    i = pl.program_id(0)
    me = lax.axis_index("dp")
    d = md.shape[2]
    rg, rd = mg.shape[1], md.shape[1]
    my_g = pl.ds(pl.multiple_of(me * rg, rg), rg)
    my_d = pl.ds(pl.multiple_of(me * rd, rd), rd)
    width = gu_ref.shape[1]
    blocks = wg.shape[2] // LANES
    last = pl.ds(2 * LANES * (blocks - 1), 2 * LANES)
    rings = [Ring(n, own_d, *ring_refs[:3])]
    for k, ((first, wide), _) in enumerate(groups):
        rings.append(Ring(n, own_gu.at[:, pl.ds(first * 2 * LANES, wide * 2 * LANES)], *ring_refs[3 * k + 3 : 3 * k + 6]))
    load = pltpu.make_async_copy(d0_hbm, own_d, in_sem.at[0])
    loads = [
        pltpu.make_async_copy(gu1, gbuf.at[1], in_sem.at[1]),
        pltpu.make_async_copy(d1, dbuf.at[1], in_sem.at[2]),
        pltpu.make_async_copy(mg, mb_g, in_sem.at[3]),
        pltpu.make_async_copy(mu, mb_u, in_sem.at[4]),
        pltpu.make_async_copy(md, mb_d, in_sem.at[5]),
        pltpu.make_async_copy(vg, vb_g, in_sem.at[6]),
        pltpu.make_async_copy(vu, vb_u, in_sem.at[7]),
        pltpu.make_async_copy(vd, vb_d, in_sem.at[8]),
        pltpu.make_async_copy(wg.at[:, my_g], wb_g.at[0], in_sem.at[9]),
        pltpu.make_async_copy(wu.at[:, my_g], wb_g.at[1], in_sem.at[10]),
        pltpu.make_async_copy(wd.at[:, my_d], wb_d, in_sem.at[11]),
    ]

    @pl.when(i == 0)
    def _():
        load.start()
        greet(n, tuple(range(1, n)))
        load.wait()
        rings[0].start()
        for c in loads:
            c.start()

    ticks(todo, rings, steps, 4, 0)
    for k, (_, at) in enumerate(groups):
        if at < steps:

            @pl.when(i == at)
            def _(k=k):
                rings[k + 1].start()

    def keep(chunk, wide, dw):
        own_gu[:, pl.ds(pl.multiple_of(chunk * width, width), wide)] = dw

    back_of_chunk(dh_ref, a_ref, gu_ref, wd_ref, dgu_ref, acc, blocks, keep, lambda k, only: ticks(todo, rings, steps, 4, k, only))

    @pl.when(i == steps - 1)
    def _():
        straight = []
        for k in range(1, n):
            to = lax.rem(me + k, n)
            straight.append(
                pltpu.make_async_remote_copy(
                    src_ref=own_gu.at[pl.ds(pl.multiple_of(to * rg, rg), rg), last],
                    dst_ref=direct.at[k - 1],
                    send_sem=direct_s.at[k - 1],
                    recv_sem=direct_r.at[k - 1],
                    device_id={"dp": to},
                    device_id_type=MESH,
                )
            )
        for c in loads:
            c.wait()
        for c in straight:
            c.start()
        rest_of_plan(todo, rings, 4 * steps)
        for c in straight:
            c.wait_recv()
        own_terms = own_gu[my_g, last].astype(F32)
        gbuf[0, :, last] = (own_terms + jnp.sum(direct[...].astype(F32), 0)).astype(BF)
        rings[0].finish(dbuf.at[0])
        for k, ((first, wide), _) in enumerate(groups):
            rings[k + 1].finish(gbuf.at[0, :, pl.ds(first * 2 * LANES, wide * 2 * LANES)])

        def squares(t):
            t = t.astype(F32)
            t = t * t
            t = jnp.sum(t.reshape(t.shape[0] // 8, 8, t.shape[1]), 0)
            return sum(t[:, k : k + LANES] for k in range(0, t.shape[1], LANES))

        sq = squares(gbuf[0]) + squares(gbuf[1]) + squares(dbuf[0]) + squares(dbuf[1])
        sq_send[...] = sq
        to_all = [
            pltpu.make_async_remote_copy(
                src_ref=sq_send,
                dst_ref=sq_all.at[k - 1],
                send_sem=sq_s.at[k - 1],
                recv_sem=sq_r.at[k - 1],
                device_id={"dp": lax.rem(me + k, n)},
                device_id_type=MESH,
            )
            for k in range(1, n)
        ]
        for c in to_all:
            c.start()
        for c in to_all:
            c.wait_recv()
        total = jnp.sum(sq + jnp.sum(sq_all[...], 0), keepdims=True)
        factor = jnp.minimum(1.0, 0.5 * lax.rsqrt(total / count + 1e-30))

        streams = rings[0].streams

        def gathered(layer, down, half, owner, to=(all_g, all_u, all_d)):
            owner = lax.rem(owner + n, n)
            if down:
                return to[2].at[layer, pl.ds(pl.multiple_of(owner * rd, rd), rd), pl.ds(half * (d // 2), d // 2)]
            return to[half].at[layer, pl.ds(pl.multiple_of(owner * rg, rg), rg)]

        def put(layer, down, s, hop):
            half, way, _ = streams[s]
            where = layer, down, half, me - way * hop
            sem = put_sem.at[layer * 2 + down, s, hop]
            return pltpu.make_async_copy(gathered(*where), gathered(*where, (out_g, out_u, out_d)), sem)

        def copy(layer, down, s, hop, owner):
            part = gathered(layer, down, streams[s][0], owner)
            return pltpu.make_async_remote_copy(
                src_ref=part,
                dst_ref=part,
                send_sem=ag_s.at[layer * 2 + down, s, hop - 1],
                recv_sem=ag_r.at[layer * 2 + down, s, hop - 1],
                device_id={"dp": lax.rem(me + streams[s][1] + n, n)},
                device_id_type=MESH,
            )

        def sending(layer, down, s, hop):
            return copy(layer, down, s, hop, me - streams[s][1] * (hop - 1))

        def arrival(layer, down, s, hop):
            return copy(layer, down, s, hop, me - streams[s][1] * hop)

        def adamw(w_ref, m_ref, v_ref, g, out):
            g = g.astype(F32) * factor
            m = 0.9 * m_ref[...] + 0.1 * g
            v = 0.95 * v_ref[...] + 0.05 * g * g
            w = w_ref[...].astype(F32)
            out[...] = (w - 0.02 * (m * lax.rsqrt(v + 1e-8) + 0.1 * w)).astype(BF)
            m_ref[...] = m
            v_ref[...] = v

        units = [(layer, down) for layer in (0, 1) for down in (0, 1)]
        for layer, down in units:
            if down:
                adamw(wb_d.at[layer], mb_d.at[layer], vb_d.at[layer], dbuf[layer], all_d.at[layer, my_d])
            else:
                for j, (m, v, to) in enumerate(((mb_g, vb_g, all_g), (mb_u, vb_u, all_u))):
                    g = [gbuf[layer, :, k : k + LANES] for k in range(j * LANES, gbuf.shape[2], 2 * LANES)]
                    adamw(wb_g.at[j, layer], m.at[layer], v.at[layer], jnp.concatenate(g, 1), to.at[layer, my_g])
            for s in range(4):
                sending(layer, down, s, 1).start()
            for s in (0, 1):
                put(layer, down, s, 0).start()
        for hop in range(1, streams[0][2] + 1):
            for layer, down in units:
                for s in range(4):
                    if hop <= streams[s][2]:
                        arrival(layer, down, s, hop).wait_recv()
                        if hop < streams[s][2]:
                            sending(layer, down, s, hop + 1).start()
                        put(layer, down, s, hop).start()
        for c in to_all + straight:
            c.wait_send()
        for layer, down in units:
            for s in range(4):
                for hop in range(1, streams[s][2] + 1):
                    sending(layer, down, s, hop).wait_send()
                for hop in range(0 if s < 2 else 1, streams[s][2] + 1):
                    put(layer, down, s, hop).wait()


def store_kernel(*refs):
    k = len(refs) // 2
    copies = [pltpu.make_async_copy(a, b, refs[-1].at[j]) for j, (a, b) in enumerate(zip(refs[:k], refs[k : 2 * k]))]
    for c in copies:
        c.start()
    for c in copies:
        c.wait()


def params(cid=None, mib=62):
    if cid is None:
        return pltpu.CompilerParams(vmem_limit_bytes=mib << 20)
    return pltpu.CompilerParams(vmem_limit_bytes=mib << 20, collective_id=cid, has_side_effects=True)


def solution(mesh):
    n = mesh.shape["dp"]
    hops = n // 2, n - 1 - n // 2

    def step(x, dy, wg, wu, wd, mg, mu, md, vg, vu, vd):
        x, dy = x[0], dy[0]
        tokens, d = x.shape
        ff = wd.shape[1]
        rg, rd = d // n, ff // n
        tile = 512
        steps = tokens // tile
        blocks = ff // LANES
        rows = lambda c: pl.BlockSpec((tile, c), lambda i: (i, 0))
        whole = lambda *s: pl.BlockSpec(s, lambda i: (0,) * len(s))
        once = lambda *s: pl.BlockSpec(s, lambda i: (0,) * len(s), pipeline_mode=pl.Buffered(1))
        array = jax.ShapeDtypeStruct
        sem, vm = pltpu.SemaphoreType.DMA, pltpu.VMEM
        mm = 2 * tokens * d * ff

        def us(row_count, cols):
            return row_count * cols * 2 / 46.6e3

        def ring(row_count, cols):
            return [vm((4, hops[0], row_count, cols // 2), BF), sem((4, hops[0])), sem((4, hops[0]))]

        gu0, s0, h1, a0, a1, dgu1, dwd1 = pl.pallas_call(
            top_kernel,
            grid=(steps,),
            in_specs=[rows(d), rows(d), ANY, ANY, ANY],
            out_specs=[rows(2 * ff), rows(ff), rows(d), rows(d), rows(d), rows(2 * ff), whole(ff, d)],
            out_shape=[array((tokens, 2 * ff), F32), array((tokens, ff), BF)]
            + [array((tokens, d), BF)] * 3
            + [array((tokens, 2 * ff), BF), array((ff, d), BF)],
            scratch_shapes=[
                vm((2, d, 2 * ff), BF), vm((2, ff, d), BF), vm((tile, ff), BF), vm((ff, d), F32), sem((2, 2 * blocks)), sem((2,)),
            ],
            compiler_params=params(),
            cost_estimate=pl.CostEstimate(flops=7 * mm, bytes_accessed=100 << 20, transcendentals=0),
            name="top",
        )(x, dy, wg, wu, wd)

        pieces = 2 * -(-blocks // 2)
        of_chunk = lambda layer: [
            once(tokens, d),
            once(tokens, d),
            pl.BlockSpec((tokens // 2, 4 * LANES), lambda i: (lax.rem(i, 2), i // 2)),
            pl.BlockSpec((1, 2 * LANES, d), lambda i: (layer, i // 2, 0)),
        ]
        columns = lambda r: pl.BlockSpec((r, 2 * LANES), lambda i: (0, i))
        dwgu1, sum_d1 = pl.pallas_call(
            functools.partial(gu_kernel, n, blocks, plan(hops, [(0, us(rd, d // 2))], blocks, 1.8)),
            grid=(blocks,),
            in_specs=[once(tokens, d), columns(tokens), ANY],
            out_specs=[columns(d), whole(rd, d)],
            out_shape=[array((d, 2 * ff), BF), array((rd, d), BF)],
            scratch_shapes=[vm((ff, d), BF), sem(())] + ring(rd, d),
            compiler_params=params(0),
            cost_estimate=pl.CostEstimate(flops=2 * mm, bytes_accessed=30 << 20, transcendentals=0),
            name="gu1",
        )(a1, dgu1, dwd1)

        cut = blocks // 2 * 2 * LANES
        parts = ((0, cut), (cut, 2 * ff - cut))
        todo = plan(hops, [(0, us(rg, w // 2)) for _, w in parts], 2 * steps, 2.0)
        dh1, dwd0, sum_gu1 = pl.pallas_call(
            functools.partial(mid_kernel, n, steps, todo, parts),
            grid=(steps,),
            in_specs=[rows(d), rows(d), rows(2 * ff), rows(ff), ANY, ANY, ANY],
            out_specs=[rows(d), whole(ff, d), whole(rg, 2 * ff)],
            out_shape=[array((tokens, d), BF), array((ff, d), BF), array((rg, 2 * ff), BF)],
            scratch_shapes=[vm((d, 2 * ff), BF), vm((ff, d), F32), sem((2 * blocks,))]
            + [vm((d, 2 * ff), BF), sem(())]
            + [r for _, w in parts for r in ring(rg, w)],
            compiler_params=params(1),
            cost_estimate=pl.CostEstimate(flops=3 * mm, bytes_accessed=50 << 20, transcendentals=0),
            name="mid",
        )(h1, dy, dgu1, s0, wg, wu, dwgu1)

        groups = [(k, min(4, blocks - 1 - k)) for k in range(0, blocks - 1, 4)]
        ready = [min(2 * -(-(f + w) // 2), pieces) for f, w in groups]
        todo = plan(hops, [(0, us(rd, d // 2))] + [(4 * at, us(rg, w * LANES)) for at, (_, w) in zip(ready, groups)], 4 * pieces, 0.85)
        outs = pl.pallas_call(
            functools.partial(end_kernel, n, pieces, todo, list(zip(groups, ready)), float(wg.size + wu.size + wd.size)),
            grid=(pieces,),
            in_specs=of_chunk(0) + [ANY] * 12,
            out_specs=[pl.BlockSpec(memory_space=pltpu.VMEM)] * 9,
            out_shape=[vm(t.shape, BF) for t in (wg, wu, wd)] + [vm(t.shape, F32) for t in (mg, mu, md, vg, vu, vd)],
            scratch_shapes=[
                vm((tokens // 2, 4 * LANES), BF), vm((d, 4 * LANES), F32), vm(wg.shape, BF), vm(wu.shape, BF), vm(wd.shape, BF),
                vm((d, 2 * ff), BF), vm((ff, d), BF), vm((2, rg, 2 * ff), BF), vm((2, rd, d), BF),
                vm((2, *mg.shape), BF), vm(md.shape, BF), vm((8, LANES), F32), vm((n - 1, 8, LANES), F32),
                sem((12,)), sem((n - 1,)), sem((n - 1,)), sem((4, 4, hops[0])), sem((4, 4, hops[0])), sem((4, 4, hops[0] + 1)),
                vm((n - 1, rg, 2 * LANES), BF), sem((n - 1,)), sem((n - 1,)),
            ] + ring(rd, d) + [r for _, w in groups for r in ring(rg, w * 2 * LANES)],
            compiler_params=params(2, 48),
            cost_estimate=pl.CostEstimate(flops=2 * mm, bytes_accessed=30 << 20, transcendentals=0),
            name="end",
        )(dh1, a0, gu0, wd, dwd0, sum_gu1, sum_d1, wg, wu, wd, mg, mu, md, vg, vu, vd)
        return tuple(
            pl.pallas_call(
                store_kernel,
                in_specs=[pl.BlockSpec(memory_space=pltpu.VMEM)] * 9,
                out_specs=[ANY] * 9,
                out_shape=[array(t.shape, t.dtype) for t in outs],
                scratch_shapes=[sem((9,))],
                compiler_params=params(None, 2),
                name="store",
            )(*outs)
        )

    seq, whole, rows = P(("rep", "dp"), None, None), P(None, None, None), P(None, "dp", None)
    return jax.shard_map(
        step,
        mesh=mesh,
        in_specs=(seq, seq) + (whole,) * 3 + (rows,) * 6,
        out_specs=(P("rep", None, None),) * 3 + (P("rep", "dp", None),) * 6,
        check_vma=False,
    )
```
